32 devices in a mesh: graph: 8 (over z, y), sample: 4 (over x, core).
Axes of the slice: x: 2, y: 2, z: 4, core: 2. Of those that a mesh axis runs over, the one named last changes fastest.
Arguments:
- grid_in: bfloat16 [4, 4096, 256], P('sample', 'graph'), may hold values from -6 to 6
- mesh_init: bfloat16 [4, 1024, 512], P('sample', 'graph'), may hold values from -6 to 6
- g2m_geometry: bfloat16 [4, 8192], P(None, 'graph'), may hold values from -6 to 6
- w_embed: bfloat16 [256, 512], replicated, may hold values from -0.375 to 0.375
- w_g2m: bfloat16 [512, 512], replicated, may hold values from -0.25 to 0.25
- w_geo: bfloat16 [4, 512], replicated, may hold values from -3 to 3
- a_send: bfloat16 [512, 512], replicated, may hold values from -0.25 to 0.25
- a_recv: bfloat16 [512, 512], replicated, may hold values from -0.25 to 0.25
- b_node: bfloat16 [512, 512], replicated, may hold values from -0.25 to 0.25
- cotangent: bfloat16 [4, 1024, 512], P('sample', 'graph'), may hold values from -6 to 6
- g2m_send_rows: int32 [8, 8, 8], P('graph'), may hold values from 0 to 511
- g2m_counts: int32 [8, 8], P('graph'), may hold values from 0 to 8, as said below
- g2m_senders: int32 [8192], P('graph'), may hold values from 0 to 63
- g2m_receivers: int32 [8192], P('graph'), may hold values from 0 to 127
- mesh_send_rows: int32 [8, 8, 4], P('graph'), may hold values from 0 to 127
- mesh_senders: int32 [4096], P('graph'), may hold values from 0 to 159
- mesh_receivers: int32 [4096], P('graph'), may hold values from 0 to 127
Outputs:
- mesh_out: bfloat16 [4, 1024, 512], P('sample', 'graph')
- grad_mesh: float32 [4, 1024, 512], P('sample', 'graph')
- grad_weights: float32 [1536, 512], P('graph')
The draws below stay inside these ranges and needn't reach their ends.
Inputs may be any that keep to these rules, and one draw needn't show every extreme that they name: `g2m_send_rows`: entry [b, g, j] is a row of band b's own 512 rows. `g2m_counts`: entry [b, g] is the number of live slots from band b to partition g; every band has some partition at 8, and some partition receives 8 from every band. `g2m_senders`: b * 8 + j names slot j from band b, for the partition that holds the edge. `g2m_receivers`: A node of the partition that holds the edge. `mesh_send_rows`: entry [b, g, j] is a row of partition b's own 128 rows. `mesh_senders`: A row of the holding partition's sender_table: below 32 a row received from another partition, else a local node. `mesh_receivers`: A node of the partition that holds the edge.
All inputs are finite; a program needn't handle non-finite values.
Results may differ from the reference program's by a relative error of at most 0.012.
The reference program's roundings to bfloat16 on the way count: a program that leaves them out, or rounds other values in their place, can miss the bound.
Values may be sent and summed in bfloat16 or wider, within the bound.
A program may use at most 64 MiB of HBM per device.

```python
import jax
import jax.numpy as jnp
from jax import lax

D = 512
GI = 256
GRID_DEV = 512
MESH_DEV = 128
G2M_DEV = 1024
EDGE_DEV = 512
CAP = 8
MCAP = 4
SAMPLES = 4
GRID = 4096
MESH = 1024
G2M = 8192
EDGES = 4096
N_GRAPH = 8


def draw_g2m_counts(key, part):
    keys = jax.random.split(jax.random.fold_in(key, 17), 4)
    row_limit = jax.random.randint(keys[0], (N_GRAPH, 1), CAP // 2, CAP + 1)
    base_counts = jax.random.randint(keys[1], (N_GRAPH, N_GRAPH), 0, CAP + 1)
    counts = jnp.minimum(base_counts, row_limit)
    order = jax.random.permutation(keys[2], N_GRAPH)
    full_column = jax.random.randint(keys[3], (), 0, N_GRAPH)
    columns = jnp.arange(N_GRAPH, dtype=jnp.int32)
    counts = jnp.where(columns[None, :] == order[:, None], CAP, counts)
    counts = jnp.where(columns[None, :] == full_column, CAP, counts)
    return counts.astype(jnp.int32)


def plant(result, rng, least, top_value):
    longest = result.shape.index(max(result.shape))
    spots = []
    for shift in (0, 1):
        where = [jax.random.randint(jax.random.fold_in(rng, axis), (), 0, length) for axis, length in enumerate(result.shape)]
        where[longest] = (where[longest] + shift) % result.shape[longest]
        spots.append(tuple(where))
    return result.at[spots[0]].set(least).at[spots[1]].set(top_value)


def with_spikes(drawn, key, source, target, blocks, factor):
    owner, partner = [(jnp.arange(drawn.shape[axis_at]) // (drawn.shape[axis_at] // blocks)).reshape([-1 if axis == axis_at else 1 for axis in range(drawn.ndim)]) for axis_at in (source, target)]
    chosen = jax.random.permutation(key, blocks)[partner]
    strong = (owner == chosen) | (owner == (partner + blocks // 2) % blocks)
    return jnp.where(strong, factor * drawn, drawn)


def level_of(key, extent, shards, low, high):
    def one(position, shards_of):
        steps = jax.random.uniform(jax.random.fold_in(jax.random.fold_in(key, 6), position), (shards_of,), jnp.float32, low / len(shards), high / len(shards))
        return jnp.repeat(jnp.exp(steps), extent[position] // shards_of).reshape((-1,) + (1,) * (len(extent) - position - 1))

    level = one(*shards[0])
    for cut in shards[1:]:
        level = level * one(*cut)
    return level


def scatter_about(own_key, extent, scale, limit, cuts=(), kind=jnp.bfloat16):
    loudness = level_of(own_key, extent, cuts, -0.22, 0.18) if cuts else 1.0
    drawn = jax.random.normal(own_key, extent, jnp.float32) * scale * loudness
    return jnp.minimum(jnp.maximum(drawn, -limit), limit).astype(kind)


def gaussian_with(stream_key, extent, scale, bound, shards, heavy, kind=jnp.bfloat16):
    drawn = scale * jax.random.normal(stream_key, extent, jnp.float32)
    if shards:
        drawn = drawn * level_of(stream_key, extent, shards, -0.22, 0.18)
    return jnp.clip(with_spikes(drawn, jax.random.fold_in(stream_key, 3), *heavy), -bound, bound).astype(kind)


def setup_inputs(seed: int = 0) -> dict:
    arg_keys = jax.random.split(jax.random.key(seed), 18)
    return {
        "grid_in": scatter_about(arg_keys[0], (SAMPLES, GRID, GI), 1.0, 6.0, ((0, 4), (1, 8))),
        "mesh_init": gaussian_with(arg_keys[1], (SAMPLES, MESH, D), 1.0, 6.0, ((0, 4), (1, 8)), (1, 2, 8, 2.0)),
        "g2m_geometry": scatter_about(arg_keys[2], (4, G2M), 1.0, 6.0, ((1, 8),)),
        "w_embed": scatter_about(arg_keys[3], (GI, D), GI ** -0.5, 0.375),
        "w_g2m": scatter_about(arg_keys[4], (D, D), D ** -0.5, 0.25),
        "w_geo": scatter_about(arg_keys[5], (4, D), 4 ** -0.5, 3.0),
        "a_send": scatter_about(arg_keys[6], (D, D), D ** -0.5, 0.25),
        "a_recv": scatter_about(arg_keys[7], (D, D), D ** -0.5, 0.25),
        "b_node": scatter_about(arg_keys[8], (D, D), D ** -0.5, 0.25),
        "cotangent": scatter_about(arg_keys[9], (SAMPLES, MESH, D), 1.0, 6.0, ((0, 4), (1, 8))),
        "g2m_send_rows": plant(jax.random.randint(arg_keys[10], (N_GRAPH, N_GRAPH, CAP), 0, GRID_DEV), jax.random.fold_in(arg_keys[10], 1), 0, GRID_DEV - 1).astype(jnp.int32),
        "g2m_counts": draw_g2m_counts(jax.random.fold_in(arg_keys[17], 71), 0),
        "g2m_senders": plant(jax.random.randint(arg_keys[12], (G2M,), 0, N_GRAPH * CAP), jax.random.fold_in(arg_keys[12], 1), 0, (N_GRAPH * CAP) - 1).astype(jnp.int32),
        "g2m_receivers": plant(jax.random.randint(arg_keys[13], (G2M,), 0, MESH_DEV), jax.random.fold_in(arg_keys[13], 1), 0, MESH_DEV - 1).astype(jnp.int32),
        "mesh_send_rows": plant(jax.random.randint(arg_keys[14], (N_GRAPH, N_GRAPH, MCAP), 0, MESH_DEV), jax.random.fold_in(arg_keys[14], 1), 0, MESH_DEV - 1).astype(jnp.int32),
        "mesh_senders": plant(jax.random.randint(arg_keys[15], (EDGES,), 0, N_GRAPH * MCAP + MESH_DEV), jax.random.fold_in(arg_keys[15], 1), 0, (N_GRAPH * MCAP + MESH_DEV) - 1).astype(jnp.int32),
        "mesh_receivers": plant(jax.random.randint(arg_keys[16], (EDGES,), 0, MESH_DEV), jax.random.fold_in(arg_keys[16], 1), 0, MESH_DEV - 1).astype(jnp.int32),
    }


def silu_slope(values):
    sigmoid_v = jax.nn.sigmoid(values)
    return sigmoid_v * (1.0 + values * (1.0 - sigmoid_v))


def segment_rows(values, index_list, segments):
    moved = jnp.moveaxis(values.astype(jnp.float32), 1, 0)
    summed = jax.ops.segment_sum(moved, index_list, num_segments=segments)
    return jnp.moveaxis(summed, 0, 1)


def flat_dot(left, right):
    product = jnp.dot(left.reshape(-1, left.shape[-1]), right, preferred_element_type=jnp.float32)
    return product.reshape(left.shape[:-1] + (right.shape[-1],))


def reference(grid_in, mesh_init, g2m_geometry, w_embed, w_g2m, w_geo, a_send, a_recv, b_node, cotangent, g2m_send_rows, g2m_counts, g2m_senders, g2m_receivers, mesh_send_rows, mesh_senders, mesh_receivers):
    sources = jnp.arange(N_GRAPH, dtype=jnp.int32)
    grid_slots = jnp.arange(CAP, dtype=jnp.int32)
    local_nodes = jnp.arange(MESH_DEV, dtype=jnp.int32)
    table_size = N_GRAPH * MCAP + MESH_DEV

    def encode(device):
        picked = (sources[:, None] * GRID_DEV + g2m_send_rows[:, device, :]).reshape(-1).astype(jnp.int32)
        live_slots = (grid_slots[None, :] < g2m_counts[:, device][:, None]).reshape(-1)
        raw_rows = grid_in[:, picked, :]
        embedded = jax.nn.silu(flat_dot(raw_rows, w_embed))
        latent = jnp.where(live_slots[None, :, None], embedded, jnp.float32(0.0)).astype(jnp.bfloat16)
        grid_proj = flat_dot(latent, w_g2m)
        senders = lax.dynamic_slice_in_dim(g2m_senders, device * G2M_DEV, G2M_DEV, 0)
        receivers = lax.dynamic_slice_in_dim(g2m_receivers, device * G2M_DEV, G2M_DEV, 0)
        geometry = lax.dynamic_slice_in_dim(g2m_geometry, device * G2M_DEV, G2M_DEV, 1)
        geo_part = jnp.dot(geometry.T, w_geo, preferred_element_type=jnp.float32)
        messages = jax.nn.silu(grid_proj[:, senders, :] + geo_part[None]).astype(jnp.bfloat16)
        own_init = lax.dynamic_slice_in_dim(mesh_init, device * MESH_DEV, MESH_DEV, 1)
        return (own_init.astype(jnp.float32) + segment_rows(messages, receivers, MESH_DEV)).astype(jnp.bfloat16)

    stacked = lax.map(encode, sources)
    mesh_latent = jnp.moveaxis(stacked, 0, 1).reshape(SAMPLES, N_GRAPH * MESH_DEV, D)

    def process(carry, device):
        extra, grad_send, grad_recv, grad_node = carry
        remote_ids = (sources[:, None] * MESH_DEV + mesh_send_rows[:, device, :]).reshape(-1).astype(jnp.int32)
        node_ids = jnp.concatenate([remote_ids, (device * MESH_DEV + local_nodes).astype(jnp.int32)])
        sender_table = mesh_latent[:, node_ids, :]
        own_latent = lax.dynamic_slice_in_dim(mesh_latent, device * MESH_DEV, MESH_DEV, 1)
        senders = lax.dynamic_slice_in_dim(mesh_senders, device * EDGE_DEV, EDGE_DEV, 0)
        receivers = lax.dynamic_slice_in_dim(mesh_receivers, device * EDGE_DEV, EDGE_DEV, 0)
        send_proj = flat_dot(sender_table, a_send)
        recv_proj = flat_dot(own_latent, a_recv)
        pre_act = send_proj[:, senders, :] + recv_proj[:, receivers, :]
        edge_out = jax.nn.silu(pre_act).astype(jnp.bfloat16)
        aggregate = segment_rows(edge_out, receivers, MESH_DEV).astype(jnp.bfloat16)
        update = flat_dot(aggregate, b_node)
        mesh_new = (own_latent.astype(jnp.float32) + jax.nn.silu(update)).astype(jnp.bfloat16)
        cot_value = lax.dynamic_slice_in_dim(cotangent, device * MESH_DEV, MESH_DEV, 1).astype(jnp.float32)
        d_update = (cot_value * silu_slope(update)).astype(jnp.bfloat16)
        d_aggregate = flat_dot(d_update, b_node.T).astype(jnp.bfloat16)
        d_pre = (d_aggregate[:, receivers, :].astype(jnp.float32) * silu_slope(pre_act)).astype(jnp.bfloat16)
        recv_grad = segment_rows(d_pre, receivers, MESH_DEV).astype(jnp.bfloat16)
        send_grad = segment_rows(d_pre, senders, table_size).astype(jnp.bfloat16)
        grad_send = grad_send + jnp.dot(sender_table.reshape(-1, D).T, send_grad.reshape(-1, D), preferred_element_type=jnp.float32)
        grad_recv = grad_recv + jnp.dot(own_latent.reshape(-1, D).T, recv_grad.reshape(-1, D), preferred_element_type=jnp.float32)
        grad_node = grad_node + jnp.dot(aggregate.reshape(-1, D).T, d_update.reshape(-1, D), preferred_element_type=jnp.float32)
        returned = flat_dot(send_grad, a_send.T)
        extra = extra.at[:, node_ids, :].add(returned)
        local_grad = cot_value + flat_dot(recv_grad, a_recv.T)
        return (extra, grad_send, grad_recv, grad_node), (mesh_new, local_grad)

    start = (jnp.zeros((SAMPLES, N_GRAPH * MESH_DEV, D), jnp.float32), jnp.zeros((D, D), jnp.float32), jnp.zeros((D, D), jnp.float32), jnp.zeros((D, D), jnp.float32))
    final, outputs = lax.scan(process, start, sources)
    extra, grad_send, grad_recv, grad_node = final
    mesh_new, local_grad = outputs
    mesh_out = jnp.moveaxis(mesh_new, 0, 1).reshape(SAMPLES, N_GRAPH * MESH_DEV, D)
    grad_mesh = jnp.moveaxis(local_grad, 0, 1).reshape(SAMPLES, N_GRAPH * MESH_DEV, D) + extra
    grad_weights = jnp.concatenate([grad_send, grad_recv, grad_node], axis=0)
    return mesh_out, grad_mesh, grad_weights
```

```python
import functools

import jax
import jax.numpy as jnp
from jax import lax
from jax.experimental import pallas as pl
from jax.experimental.pallas import tpu as pltpu
from jax.sharding import PartitionSpec as P

PAD = 8
TILE = 16
COLUMNS = 2
BF = jnp.bfloat16
F32 = jnp.float32


def logistic(v):
    return 0.5 + 0.5 * jnp.tanh(0.5 * v)


def dot(left, right):
    return jnp.dot(left, right, preferred_element_type=F32)


def times_transposed(left, right):
    return lax.dot_general(left, right, (((1,), (1,)), ((), ())), preferred_element_type=F32)


def inner_rows(left, right):
    return lax.dot_general(left, right, (((0,), (0,)), ((), ())), preferred_element_type=F32)


def hot(rows, index_row):
    shape = (rows, index_row.shape[1])
    return jnp.where(lax.broadcasted_iota(jnp.int32, shape, 0) == index_row, 1.0, 0.0).astype(BF)


def two_terms(values):
    high = values.astype(BF)
    return jnp.concatenate([high, (values - high.astype(F32)).astype(BF)], axis=0)


def repack(position, count):
    return position if count == PAD else position + lax.div(position, count) * (PAD - count)


def spread(table, pattern):
    low = lax.rem(table, 256)
    return dot(lax.div(table, 256).astype(BF), pattern) * 256.0 + dot(low.astype(BF), pattern)


def slot_rows(grid_rows_ref, counts_ref, halo_rows_ref, groups, padded, halos):
    def grid_of(rows):
        row = lax.broadcasted_iota(jnp.int32, (rows, padded), 0)
        return row, lax.broadcasted_iota(jnp.int32, (rows, padded), 1)

    peer, column = grid_of(groups)
    by_peer = lax.div(column, PAD) == peer
    peer_hot = jnp.where(by_peer, 1.0, 0.0).astype(BF)
    slot, column = grid_of(grid_rows_ref.shape[2])
    slot_hot = jnp.where(lax.rem(column, PAD) == slot, 1.0, 0.0).astype(BF)
    picked = jnp.sum(jnp.where(by_peer, spread(grid_rows_ref[0], slot_hot), 0.0), axis=0, keepdims=True)
    live = dot(counts_ref[...].astype(BF), peer_hot)
    _, column = grid_of(1)
    position = lax.rem(column, PAD)
    grid_rows = jnp.where(position.astype(F32) < live, picked, -1.0).astype(jnp.int32)
    slot, column = grid_of(halos)
    by_slot = lax.rem(column, PAD) == slot
    picked = jnp.sum(jnp.where(by_slot, spread(halo_rows_ref[0], peer_hot), 0.0), axis=0, keepdims=True)
    halo_rows = jnp.where(position < halos, picked, -1.0).astype(jnp.int32)
    return grid_rows, halo_rows


def kernel(
    cfg,
    grid_rows_ref, counts_ref, halo_rows_ref, g2m_senders_ref, g2m_receivers_ref, mesh_senders_ref, mesh_receivers_ref,
    geom_ref, w_geo_ref,
    grid_hbm, init_hbm, w_embed_hbm, w_g2m_hbm, a_send_hbm, a_recv_hbm, b_node_hbm, cot_hbm,
    out_ref, grad_ref, weights_ref,
    grid_v, init_v, w_embed_v, w_g2m_v, a_send_v, a_recv_v, b_node_v, cot_v,
    lat_send, lat_recv, halo_send, halo_recv, back_send, back_recv,
    geo_part, slope_v, local_grad, grads, pair_recv, staged, plane_recv, line_send, line_recv, last_send, last_recv,
    load_sem, g_send_sem, g_recv_sem, pair_sem, plane_sem, line_sem, last_sem,
):
    groups, slots, halos, fused = cfg
    me = lax.axis_index("graph")
    sample = lax.axis_index("sample")
    half = lax.rem(sample, 2)
    far = lax.div(sample, 2)
    column = lax.rem(me, COLUMNS)
    line = lax.div(me, COLUMNS)
    core_peer = sample + 1 - 2 * half

    def sample_at(dx, dc):
        return 2 * lax.rem(far + dx, 2) + lax.rem(half + dc, 2)

    loads = []
    for i, (src, dst) in enumerate(
        [
            (grid_hbm.at[0], grid_v), (w_embed_hbm, w_embed_v), (w_g2m_hbm, w_g2m_v),
            (init_hbm.at[0], init_v), (a_send_hbm, a_send_v), (a_recv_hbm, a_recv_v),
            (b_node_hbm, b_node_v), (cot_hbm.at[0], cot_v),
        ]
    ):
        copy = pltpu.make_async_copy(src, dst, load_sem.at[i])
        if i < 4:
            copy.start()
        loads.append(copy)
    ld_grid, ld_embed, ld_g2m, ld_init, ld_asend, ld_arecv, ld_bnode, ld_cot = loads

    barrier = pltpu.get_barrier_semaphore()

    def greet(step, carry):
        pl.semaphore_signal(barrier, inc=1, device_id={"graph": lax.rem(me + step, groups)}, device_id_type=pl.DeviceIdType.MESH)
        return carry

    lax.fori_loop(1, groups, greet, 0)
    greeted = groups - 1
    if fused:
        other_column = COLUMNS * line + lax.rem(column + 1, COLUMNS)
        for graph, peer in ((me, core_peer), (me, sample_at(1, 0)), (me, sample_at(1, 1)), (other_column, sample_at(1, 0))):
            pl.semaphore_signal(
                barrier, inc=1, device_id={"graph": graph, "sample": peer}, device_id_type=pl.DeviceIdType.MESH
            )
        greeted += 4

    def swap_copy(kind, src, dst, peer, slot):
        return pltpu.make_async_remote_copy(
            src_ref=src, dst_ref=dst, send_sem=g_send_sem.at[kind, peer], recv_sem=g_recv_sem.at[kind, slot],
            device_id={"graph": peer}, device_id_type=pl.DeviceIdType.MESH,
        )

    def swap_start(kind, source, target):
        def body(step, carry):
            peer = lax.rem(me + step, groups)
            swap_copy(kind, source.at[peer], target.at[me], peer, me).start()
            return carry

        lax.fori_loop(1, groups, body, 0)

    def swap_wait(kind, source, target):
        def body(step, carry):
            peer = lax.rem(me + step, groups)
            swap_copy(kind, source.at[peer], target.at[peer], peer, peer).wait()
            return carry

        lax.fori_loop(1, groups, body, 0)

    width = w_g2m_v.shape[1]
    mesh_rows = init_v.shape[0]
    padded = groups * PAD
    grid_rows, halo_rows = slot_rows(grid_rows_ref, counts_ref, halo_rows_ref, groups, padded, halos)

    pick_grid = hot(grid_v.shape[0], grid_rows)
    ld_grid.wait()
    chosen = inner_rows(pick_grid, grid_v[...]).astype(BF)
    ld_embed.wait()
    for copy in loads[4:]:
        copy.start()
    embedded = dot(chosen, w_embed_v[...])
    lat_send[...] = (embedded * logistic(embedded)).astype(BF).reshape(groups, PAD, width)
    pl.semaphore_wait(barrier, greeted)
    swap_start(0, lat_send, lat_recv)
    lat_recv[me] = lat_send[me]
    geo_part[...] = inner_rows(geom_ref[...], w_geo_ref[...])
    grid_hot = hot(padded, repack(g2m_senders_ref[...], slots))
    recv_hot_g = hot(mesh_rows, g2m_receivers_ref[...])
    ld_g2m.wait()
    ld_init.wait()
    swap_wait(0, lat_send, lat_recv)
    grid_proj = dot(lat_recv[...].reshape(padded, width), w_g2m_v[...])
    grid_proj = two_terms(grid_proj)
    grid_hot = jnp.concatenate([grid_hot, grid_hot], axis=0)
    summed = init_v[...].astype(F32)
    edges = grid_hot.shape[1]
    chunk = 256 if edges % 256 == 0 else edges
    for first in range(0, edges, chunk):
        v = inner_rows(grid_hot[:, first : first + chunk], grid_proj) + geo_part[first : first + chunk, :]
        message = (v * logistic(v)).astype(BF)
        summed = summed + dot(recv_hot_g[:, first : first + chunk], message)
    latent = summed.astype(BF)

    pick_halo = hot(mesh_rows, halo_rows)
    halo_send[...] = inner_rows(pick_halo, latent).astype(BF).reshape(groups, PAD, width)
    swap_start(1, halo_send, halo_recv)
    halo_recv[me] = halo_send[me]
    ld_asend.wait()
    ld_arecv.wait()
    recv_proj = dot(latent, a_recv_v[...])
    local_proj = dot(latent, a_send_v[...])
    recv_hot = hot(mesh_rows, mesh_receivers_ref[...])
    table_row = mesh_senders_ref[...]
    table_row = jnp.where(
        table_row < groups * halos, repack(table_row, halos), table_row + (padded - groups * halos)
    )
    send_hot = hot(padded + mesh_rows, table_row)
    ld_bnode.wait()
    ld_cot.wait()
    swap_wait(1, halo_send, halo_recv)
    halo = halo_recv[...].reshape(padded, width)
    halo_proj = dot(halo, a_send_v[...])
    all_proj = two_terms(jnp.concatenate([halo_proj, local_proj, recv_proj], axis=0))
    all_hot = jnp.concatenate([send_hot, recv_hot], axis=0)
    twice_hot = jnp.concatenate([all_hot, all_hot], axis=0)
    mesh_edges = recv_hot.shape[1]
    chunk = 256 if mesh_edges % 256 == 0 else mesh_edges
    agg = jnp.zeros((mesh_rows, width), F32)
    for first in range(0, mesh_edges, chunk):
        v = inner_rows(twice_hot[:, first : first + chunk], all_proj)
        s = logistic(v)
        slope_v[first : first + chunk, :] = s * (1.0 + v * (1.0 - s))
        agg = agg + dot(recv_hot[:, first : first + chunk], (v * s).astype(BF))
    aggregate = agg.astype(BF)
    update = dot(aggregate, b_node_v[...])
    s = logistic(update)
    out_ref[0] = (latent.astype(F32) + update * s).astype(BF)
    cot = cot_v[...].astype(F32)
    d_update = (cot * (s * (1.0 + update * (1.0 - s)))).astype(BF)
    d_aggregate = times_transposed(d_update, b_node_v[...]).astype(BF)

    kind = BF if fused else F32
    target = grads if fused else weights_ref
    unit = staged.shape[1]
    waiting = list(range(groups))

    def rows_of(block, side):
        return pl.ds(pl.multiple_of((2 * block + side) * unit, TILE), unit)

    def pair_copy(block):
        return pltpu.make_async_remote_copy(
            src_ref=grads.at[rows_of(block, 1 - half)], dst_ref=pair_recv.at[block],
            send_sem=pair_sem.at[0, block], recv_sem=pair_sem.at[1, block],
            device_id={"sample": core_peer}, device_id_type=pl.DeviceIdType.MESH,
        )

    def store_part(number, value):
        target[number * width : (number + 1) * width, :] = value.astype(kind)

    def send_pairs(ready_from):
        while waiting and waiting[-1] * 2 * unit >= ready_from:
            pair_copy(waiting.pop()).start()

    quarter = unit // 2
    lines = groups // COLUMNS
    steps = [(1, 0), (0, 1), (1, 1)]

    def plane_copy(row, k):
        dx, dy = steps[k]
        x, y = lax.rem(far + dx, 2), lax.rem(column + dy, COLUMNS)
        return pltpu.make_async_remote_copy(
            src_ref=staged.at[COLUMNS * row + y, pl.ds(pl.multiple_of(x * quarter, TILE), quarter)],
            dst_ref=plane_recv.at[row, k],
            send_sem=plane_sem.at[0, row, k], recv_sem=plane_sem.at[1, row, k],
            device_id={"graph": COLUMNS * line + y, "sample": 2 * x + half}, device_id_type=pl.DeviceIdType.MESH,
        )

    def line_copy(row, slot):
        return pltpu.make_async_remote_copy(
            src_ref=line_send.at[row], dst_ref=line_recv.at[slot],
            send_sem=line_sem.at[0, row], recv_sem=line_sem.at[1, slot],
            device_id={"graph": COLUMNS * row + column}, device_id_type=pl.DeviceIdType.MESH,
        )

    def last_copy(k):
        return pltpu.make_async_remote_copy(
            src_ref=last_send, dst_ref=last_recv.at[k],
            send_sem=last_sem.at[0, k], recv_sem=last_sem.at[1, k],
            device_id={"sample": sample_at(*steps[k])}, device_id_type=pl.DeviceIdType.MESH,
        )

    def stage_row(row):
        for block in range(COLUMNS * row, COLUMNS * (row + 1)):
            pair_copy(block).wait()
            staged[block] = (grads[rows_of(block, half), :].astype(F32) + pair_recv[block].astype(F32)).astype(BF)
        for k in (2, 0, 1):
            plane_copy(row, k).start()

    store_part(2, inner_rows(aggregate, d_update))
    if fused:
        send_pairs(2 * width)
    d_both = jnp.zeros((padded + 2 * mesh_rows, width), F32)
    for first in range(0, mesh_edges, chunk):
        d_pre = (inner_rows(recv_hot[:, first : first + chunk], d_aggregate) * slope_v[first : first + chunk, :]).astype(BF)
        d_both = d_both + dot(all_hot[:, first : first + chunk], d_pre)
    d_both = d_both.astype(BF)
    halo_grad = d_both[:padded]
    send_grad = d_both[padded : padded + mesh_rows]
    recv_grad = d_both[padded + mesh_rows :]
    back_send[...] = times_transposed(halo_grad, a_send_v[...]).astype(BF).reshape(groups, PAD, width)
    swap_start(2, back_send, back_recv)
    back_recv[me] = back_send[me]
    if fused:
        stage_row(lines - 1)

    def finish_mesh():
        local_grad[...] = cot + times_transposed(recv_grad, a_recv_v[...]) + times_transposed(send_grad, a_send_v[...])
        swap_wait(2, back_send, back_recv)
        grad_ref[0] = local_grad[...] + dot(pick_halo, back_recv[...].reshape(padded, width))

    if not fused:
        store_part(1, inner_rows(latent, recv_grad))
        store_part(0, inner_rows(halo, halo_grad) + inner_rows(latent, send_grad))
        finish_mesh()
        return

    store_part(1, inner_rows(latent, recv_grad))
    send_pairs(width)
    store_part(0, inner_rows(halo, halo_grad) + inner_rows(latent, send_grad))
    send_pairs(0)
    order = [lines - 1, lines - 2] + list(range(lines - 2))
    for row in order[1:]:
        stage_row(row)
    finish_mesh()

    own_rows = pl.ds(pl.multiple_of(far * quarter, TILE), quarter)
    for row in order:
        total = staged[COLUMNS * row + column, own_rows, :].astype(F32)
        for k in range(3):
            plane_copy(row, k).wait()
            total = total + plane_recv[row, k].astype(F32)
        line_send[row] = total.astype(BF)

        @pl.when(line != row)
        def _():
            line_copy(row, line).start()

    total = line_send[line].astype(F32)
    for step in range(1, lines):
        row = lax.rem(line + step, lines)
        line_copy(row, row).wait()
        total = total + line_recv[row].astype(F32)
    last_send[...] = total.astype(BF)
    for k in (2, 0, 1):
        last_copy(k).start()

    def place(k, value):
        dx, dc = steps[k] if k >= 0 else (0, 0)
        start = lax.rem(half + dc, 2) * unit + lax.rem(far + dx, 2) * quarter
        weights_ref[pl.ds(pl.multiple_of(start, TILE), quarter), :] = value

    place(-1, total)
    for k in (1, 0, 2):
        last_copy(k).wait()
        place(k, last_recv[k].astype(F32))


def hand_over(*refs):
    sources, targets, held, sem = refs[:3], refs[3:6], refs[6:9], refs[9]
    inward = [pltpu.make_async_copy(sources[i], held[i], sem.at[i]) for i in range(3)]
    outward = [pltpu.make_async_copy(held[i], targets[i], sem.at[3 + i]) for i in range(3)]
    for copy in inward:
        copy.start()
    for i in range(3):
        inward[i].wait()
        outward[i].start()
    for copy in outward:
        copy.wait()


def on_device(
    grid_in, mesh_init, g2m_geometry, w_embed, w_g2m, w_geo, a_send, a_recv, b_node, cotangent,
    g2m_send_rows, g2m_counts, g2m_senders, g2m_receivers, mesh_send_rows, mesh_senders, mesh_receivers,
):
    groups = lax.axis_size("graph")
    samples = lax.axis_size("sample")
    slots = g2m_send_rows.shape[2]
    halos = mesh_send_rows.shape[2]
    width = w_g2m.shape[1]
    mesh_rows = mesh_init.shape[1]
    block_rows = 3 * width // groups
    fused = samples == 4 and groups % COLUMNS == 0 and groups > 2 * COLUMNS and block_rows % (4 * TILE) == 0
    unit = block_rows // 2 if fused else TILE
    weights_shape = (block_rows, width) if fused else (3 * width, width)
    edges, mesh_edges = g2m_senders.shape[0], mesh_senders.shape[0]
    one = groups if fused else 1
    quarter = unit // 2 if fused else TILE
    lines = groups // COLUMNS if fused else 1
    vmem = pl.BlockSpec(memory_space=pltpu.VMEM)
    hbm = pl.BlockSpec(memory_space=pl.ANY)
    slab = pltpu.VMEM((groups, PAD, width), BF)
    mesh_out, grad_mesh, weights = pl.pallas_call(
        functools.partial(kernel, (groups, slots, halos, fused)),
        out_shape=(
            jax.ShapeDtypeStruct(mesh_init.shape, BF),
            jax.ShapeDtypeStruct(mesh_init.shape, F32),
            jax.ShapeDtypeStruct(weights_shape, F32),
        ),
        in_specs=[vmem] * 9 + [hbm] * 8,
        out_specs=(vmem, vmem, vmem),
        scratch_shapes=[
            pltpu.VMEM(grid_in.shape[1:], BF), pltpu.VMEM(mesh_init.shape[1:], BF),
            pltpu.VMEM(w_embed.shape, BF), pltpu.VMEM(w_g2m.shape, BF), pltpu.VMEM(a_send.shape, BF),
            pltpu.VMEM(a_recv.shape, BF), pltpu.VMEM(b_node.shape, BF), pltpu.VMEM(cotangent.shape[1:], BF),
            slab, slab, slab, slab, slab, slab,
            pltpu.VMEM((edges, width), F32), pltpu.VMEM((mesh_edges, width), F32),
            pltpu.VMEM((mesh_rows, width), F32),
            pltpu.VMEM((3 * width, width) if fused else (TILE, width), BF),
            pltpu.VMEM((one, unit, width), BF), pltpu.VMEM((one, unit, width), BF),
            pltpu.VMEM((lines, 3, quarter, width), BF), pltpu.VMEM((lines, quarter, width), BF),
            pltpu.VMEM((lines, quarter, width), BF), pltpu.VMEM((quarter, width), BF), pltpu.VMEM((3, quarter, width), BF),
            pltpu.SemaphoreType.DMA((8,)), pltpu.SemaphoreType.DMA((3, groups)), pltpu.SemaphoreType.DMA((3, groups)),
            pltpu.SemaphoreType.DMA((2, groups)), pltpu.SemaphoreType.DMA((2, lines, 3)),
            pltpu.SemaphoreType.DMA((2, lines)), pltpu.SemaphoreType.DMA((2, 3)),
        ],
        compiler_params=pltpu.CompilerParams(
            collective_id=0, has_side_effects=True, vmem_limit_bytes=60 * 1024 * 1024
        ),
    )(
        g2m_send_rows, g2m_counts, jnp.swapaxes(mesh_send_rows, 1, 2), g2m_senders[None], g2m_receivers[None],
        mesh_senders[None], mesh_receivers[None], g2m_geometry, w_geo, grid_in, mesh_init, w_embed, w_g2m, a_send, a_recv, b_node, cotangent,
    )
    if not fused:
        weights = lax.psum(lax.psum_scatter(weights, "graph", scatter_dimension=0, tiled=True), "sample")
        return mesh_out, grad_mesh, weights
    results = (mesh_out, grad_mesh, weights)
    return pl.pallas_call(
        hand_over,
        out_shape=tuple(jax.ShapeDtypeStruct(value.shape, value.dtype) for value in results),
        in_specs=[hbm] * 3,
        out_specs=(hbm,) * 3,
        scratch_shapes=[pltpu.VMEM(value.shape, value.dtype) for value in results] + [pltpu.SemaphoreType.DMA((6,))],
    )(*results)


def solution(mesh):
    rows = P("sample", "graph", None)
    placed = (
        rows, rows, P(None, "graph"), P(), P(), P(), P(), P(), P(), rows,
        P("graph", None, None), P("graph", None), P("graph"), P("graph"), P("graph", None, None), P("graph"), P("graph"),
    )
    return jax.shard_map(
        on_device, mesh=mesh, in_specs=placed, out_specs=(rows, rows, P("graph", None)), check_vma=False
    )
```

```python
import functools

import jax
import jax.numpy as jnp
from jax import lax
from jax.experimental import pallas as pl
from jax.experimental.pallas import tpu as pltpu
from jax.sharding import PartitionSpec as P

PAD = 8
TILE = 16
LIMIT = 67043328 - 1024 * 1024
COLUMNS = 2
BF = jnp.bfloat16
F32 = jnp.float32


def logistic(v):
    return 0.5 + 0.5 * jnp.tanh(0.5 * v)


def dot(left, right):
    return jnp.dot(left, right, preferred_element_type=F32)


def times_transposed(left, right):
    return lax.dot_general(left, right, (((1,), (1,)), ((), ())), preferred_element_type=F32)


def inner_rows(left, right):
    return lax.dot_general(left, right, (((0,), (0,)), ((), ())), preferred_element_type=F32)


def hot(rows, index_row):
    shape = (rows, index_row.shape[1])
    return jnp.where(lax.broadcasted_iota(jnp.int32, shape, 0) == index_row, 1.0, 0.0).astype(BF)


def two_terms(values):
    high = values.astype(BF)
    return jnp.concatenate([high, (values - high.astype(F32)).astype(BF)], axis=0)


def repack(position, count):
    return position if count == PAD else position + lax.div(position, count) * (PAD - count)


def spread(table, pattern):
    low = lax.rem(table, 256)
    return dot(lax.div(table, 256).astype(BF), pattern) * 256.0 + dot(low.astype(BF), pattern)


def slot_rows(grid_rows_ref, counts_ref, halo_rows_ref, groups, padded, halos):
    def grid_of(rows):
        row = lax.broadcasted_iota(jnp.int32, (rows, padded), 0)
        return row, lax.broadcasted_iota(jnp.int32, (rows, padded), 1)

    peer, column = grid_of(groups)
    by_peer = lax.div(column, PAD) == peer
    peer_hot = jnp.where(by_peer, 1.0, 0.0).astype(BF)
    slot, column = grid_of(grid_rows_ref.shape[2])
    slot_hot = jnp.where(lax.rem(column, PAD) == slot, 1.0, 0.0).astype(BF)
    picked = jnp.sum(jnp.where(by_peer, spread(grid_rows_ref[0], slot_hot), 0.0), axis=0, keepdims=True)
    live = dot(counts_ref[...].astype(BF), peer_hot)
    _, column = grid_of(1)
    position = lax.rem(column, PAD)
    grid_rows = jnp.where(position.astype(F32) < live, picked, -1.0).astype(jnp.int32)
    slot, column = grid_of(halos)
    by_slot = lax.rem(column, PAD) == slot
    picked = jnp.sum(jnp.where(by_slot, spread(halo_rows_ref[0], peer_hot), 0.0), axis=0, keepdims=True)
    halo_rows = jnp.where(position < halos, picked, -1.0).astype(jnp.int32)
    return grid_rows, halo_rows


def kernel(
    cfg,
    grid_rows_hbm, counts_hbm, halo_rows_hbm, g2m_senders_hbm, g2m_receivers_hbm, mesh_senders_hbm, mesh_receivers_hbm,
    geom_hbm, w_geo_hbm,
    grid_hbm, init_hbm, w_embed_hbm, w_g2m_hbm, a_send_hbm, a_recv_hbm, b_node_hbm, cot_hbm,
    out_ref, grad_ref, weights_ref,
    grid_rows_ref, counts_ref, halo_rows_ref, g2m_senders_ref, g2m_receivers_ref, mesh_senders_ref, mesh_receivers_ref,
    geom_ref, w_geo_ref,
    grid_v, init_v, w_embed_v, w_g2m_v, a_send_v, a_recv_v, b_node_v, cot_v,
    lat_send, lat_recv, halo_send, halo_recv, back_send, back_recv,
    geo_part, slope_v, local_grad, grads, pair_recv, staged, plane_recv, line_send, line_recv, last_send, last_recv,
    load_sem, small_sem, g_send_sem, g_recv_sem, pair_sem, plane_sem, line_sem, last_sem,
):
    groups, slots, halos, fused = cfg
    me = lax.axis_index("graph")
    sample = lax.axis_index("sample")
    half = lax.rem(sample, 2)
    far = lax.div(sample, 2)
    column = lax.rem(me, COLUMNS)
    line = lax.div(me, COLUMNS)
    core_peer = sample + 1 - 2 * half

    def sample_at(dx, dc):
        return 2 * lax.rem(far + dx, 2) + lax.rem(half + dc, 2)

    small = [
        pltpu.make_async_copy(src, dst, small_sem.at[i])
        for i, (src, dst) in enumerate(
            [
                (grid_rows_hbm, grid_rows_ref), (counts_hbm, counts_ref), (halo_rows_hbm, halo_rows_ref),
                (g2m_senders_hbm, g2m_senders_ref), (g2m_receivers_hbm, g2m_receivers_ref),
                (mesh_senders_hbm, mesh_senders_ref), (mesh_receivers_hbm, mesh_receivers_ref),
                (geom_hbm, geom_ref), (w_geo_hbm, w_geo_ref),
            ]
        )
    ]
    for copy in small[:3]:
        copy.start()
    loads = []
    for i, (src, dst) in enumerate(
        [
            (grid_hbm.at[0], grid_v), (w_embed_hbm, w_embed_v), (w_g2m_hbm, w_g2m_v),
            (init_hbm.at[0], init_v), (a_send_hbm, a_send_v), (a_recv_hbm, a_recv_v),
            (b_node_hbm, b_node_v), (cot_hbm.at[0], cot_v),
        ]
    ):
        copy = pltpu.make_async_copy(src, dst, load_sem.at[i])
        if i < 2:
            copy.start()
        loads.append(copy)
    ld_grid, ld_embed, ld_g2m, ld_init, ld_asend, ld_arecv, ld_bnode, ld_cot = loads

    barrier = pltpu.get_barrier_semaphore()

    def greet(step, carry):
        pl.semaphore_signal(barrier, inc=1, device_id={"graph": lax.rem(me + step, groups)}, device_id_type=pl.DeviceIdType.MESH)
        return carry

    lax.fori_loop(1, groups, greet, 0)
    greeted = groups - 1
    if fused:
        other_column = COLUMNS * line + lax.rem(column + 1, COLUMNS)
        for graph, peer in ((me, core_peer), (me, sample_at(1, 0)), (me, sample_at(1, 1)), (other_column, sample_at(1, 0))):
            pl.semaphore_signal(
                barrier, inc=1, device_id={"graph": graph, "sample": peer}, device_id_type=pl.DeviceIdType.MESH
            )
        greeted += 4

    def swap_copy(kind, src, dst, peer, slot):
        return pltpu.make_async_remote_copy(
            src_ref=src, dst_ref=dst, send_sem=g_send_sem.at[kind, peer], recv_sem=g_recv_sem.at[kind, slot],
            device_id={"graph": peer}, device_id_type=pl.DeviceIdType.MESH,
        )

    def swap_start(kind, source, target):
        def body(step, carry):
            peer = lax.rem(me + step, groups)
            swap_copy(kind, source.at[peer], target.at[me], peer, me).start()
            return carry

        lax.fori_loop(1, groups, body, 0)

    def swap_wait(kind, source, target):
        def body(step, carry):
            peer = lax.rem(me + step, groups)
            swap_copy(kind, source.at[peer], target.at[peer], peer, peer).wait()
            return carry

        lax.fori_loop(1, groups, body, 0)

    width = w_g2m_v.shape[1]
    mesh_rows = init_v.shape[0]
    padded = groups * PAD
    for copy in small[:3]:
        copy.wait()
    for copy in small[3:] + loads[2:4]:
        copy.start()
    grid_rows, halo_rows = slot_rows(grid_rows_ref, counts_ref, halo_rows_ref, groups, padded, halos)

    pick_grid = hot(grid_v.shape[0], grid_rows)
    ld_grid.wait()
    chosen = inner_rows(pick_grid, grid_v[...]).astype(BF)
    ld_embed.wait()
    for copy in loads[4:]:
        copy.start()
    embedded = dot(chosen, w_embed_v[...])
    lat_send[...] = (embedded * logistic(embedded)).astype(BF).reshape(groups, PAD, width)
    pl.semaphore_wait(barrier, greeted)
    swap_start(0, lat_send, lat_recv)
    lat_recv[me] = lat_send[me]
    for copy in small[3:]:
        copy.wait()
    geo_part[...] = inner_rows(geom_ref[...], w_geo_ref[...])
    grid_hot = hot(padded, repack(g2m_senders_ref[...], slots))
    recv_hot_g = hot(mesh_rows, g2m_receivers_ref[...])
    ld_g2m.wait()
    ld_init.wait()
    swap_wait(0, lat_send, lat_recv)
    grid_proj = dot(lat_recv[...].reshape(padded, width), w_g2m_v[...])
    grid_proj = two_terms(grid_proj)
    grid_hot = jnp.concatenate([grid_hot, grid_hot], axis=0)
    summed = init_v[...].astype(F32)
    edges = grid_hot.shape[1]
    chunk = 256 if edges % 256 == 0 else edges
    for first in range(0, edges, chunk):
        v = inner_rows(grid_hot[:, first : first + chunk], grid_proj) + geo_part[first : first + chunk, :]
        message = (v * logistic(v)).astype(BF)
        summed = summed + dot(recv_hot_g[:, first : first + chunk], message)
    latent = summed.astype(BF)

    pick_halo = hot(mesh_rows, halo_rows)
    halo_send[...] = inner_rows(pick_halo, latent).astype(BF).reshape(groups, PAD, width)
    swap_start(1, halo_send, halo_recv)
    halo_recv[me] = halo_send[me]
    ld_asend.wait()
    ld_arecv.wait()
    recv_proj = dot(latent, a_recv_v[...])
    local_proj = dot(latent, a_send_v[...])
    recv_hot = hot(mesh_rows, mesh_receivers_ref[...])
    table_row = mesh_senders_ref[...]
    table_row = jnp.where(
        table_row < groups * halos, repack(table_row, halos), table_row + (padded - groups * halos)
    )
    send_hot = hot(padded + mesh_rows, table_row)
    ld_bnode.wait()
    ld_cot.wait()
    swap_wait(1, halo_send, halo_recv)
    halo = halo_recv[...].reshape(padded, width)
    halo_proj = dot(halo, a_send_v[...])
    all_proj = two_terms(jnp.concatenate([halo_proj, local_proj, recv_proj], axis=0))
    all_hot = jnp.concatenate([send_hot, recv_hot], axis=0)
    twice_hot = jnp.concatenate([all_hot, all_hot], axis=0)
    mesh_edges = recv_hot.shape[1]
    chunk = 256 if mesh_edges % 256 == 0 else mesh_edges
    agg = jnp.zeros((mesh_rows, width), F32)
    for first in range(0, mesh_edges, chunk):
        v = inner_rows(twice_hot[:, first : first + chunk], all_proj)
        s = logistic(v)
        slope_v[first : first + chunk, :] = s * (1.0 + v * (1.0 - s))
        agg = agg + dot(recv_hot[:, first : first + chunk], (v * s).astype(BF))
    aggregate = agg.astype(BF)
    update = dot(aggregate, b_node_v[...])
    s = logistic(update)
    out_ref[0] = (latent.astype(F32) + update * s).astype(BF)
    cot = cot_v[...].astype(F32)
    d_update = (cot * (s * (1.0 + update * (1.0 - s)))).astype(BF)
    d_aggregate = times_transposed(d_update, b_node_v[...]).astype(BF)

    kind = BF if fused else F32
    target = grads if fused else weights_ref
    unit = staged.shape[1]
    waiting = list(range(groups))

    def rows_of(block, side):
        return pl.ds(pl.multiple_of((2 * block + side) * unit, TILE), unit)

    def pair_copy(block):
        return pltpu.make_async_remote_copy(
            src_ref=grads.at[rows_of(block, 1 - half)], dst_ref=pair_recv.at[block],
            send_sem=pair_sem.at[0, block], recv_sem=pair_sem.at[1, block],
            device_id={"sample": core_peer}, device_id_type=pl.DeviceIdType.MESH,
        )

    def store_part(number, value):
        target[number * width : (number + 1) * width, :] = value.astype(kind)

    def send_pairs(ready_from):
        while waiting and waiting[-1] * 2 * unit >= ready_from:
            pair_copy(waiting.pop()).start()

    quarter = unit // 2
    lines = groups // COLUMNS
    steps = [(1, 0), (0, 1), (1, 1)]

    def plane_copy(row, k):
        dx, dy = steps[k]
        x, y = lax.rem(far + dx, 2), lax.rem(column + dy, COLUMNS)
        return pltpu.make_async_remote_copy(
            src_ref=staged.at[COLUMNS * row + y, pl.ds(pl.multiple_of(x * quarter, TILE), quarter)],
            dst_ref=plane_recv.at[row, k],
            send_sem=plane_sem.at[0, row, k], recv_sem=plane_sem.at[1, row, k],
            device_id={"graph": COLUMNS * line + y, "sample": 2 * x + half}, device_id_type=pl.DeviceIdType.MESH,
        )

    def line_copy(row, slot):
        return pltpu.make_async_remote_copy(
            src_ref=line_send.at[row], dst_ref=line_recv.at[slot],
            send_sem=line_sem.at[0, row], recv_sem=line_sem.at[1, slot],
            device_id={"graph": COLUMNS * row + column}, device_id_type=pl.DeviceIdType.MESH,
        )

    def last_copy(k):
        return pltpu.make_async_remote_copy(
            src_ref=last_send, dst_ref=last_recv.at[k],
            send_sem=last_sem.at[0, k], recv_sem=last_sem.at[1, k],
            device_id={"sample": sample_at(*steps[k])}, device_id_type=pl.DeviceIdType.MESH,
        )

    def stage_row(row):
        for block in range(COLUMNS * row, COLUMNS * (row + 1)):
            pair_copy(block).wait()
            staged[block] = (grads[rows_of(block, half), :].astype(F32) + pair_recv[block].astype(F32)).astype(BF)
        for k in (2, 0, 1):
            plane_copy(row, k).start()

    store_part(2, inner_rows(aggregate, d_update))
    if fused:
        send_pairs(2 * width)
    d_both = jnp.zeros((padded + 2 * mesh_rows, width), F32)
    for first in range(0, mesh_edges, chunk):
        d_pre = (inner_rows(recv_hot[:, first : first + chunk], d_aggregate) * slope_v[first : first + chunk, :]).astype(BF)
        d_both = d_both + dot(all_hot[:, first : first + chunk], d_pre)
    d_both = d_both.astype(BF)
    halo_grad = d_both[:padded]
    send_grad = d_both[padded : padded + mesh_rows]
    recv_grad = d_both[padded + mesh_rows :]
    back_send[...] = times_transposed(halo_grad, a_send_v[...]).astype(BF).reshape(groups, PAD, width)
    swap_start(2, back_send, back_recv)
    back_recv[me] = back_send[me]
    if fused:
        stage_row(lines - 1)

    def finish_mesh():
        local_grad[...] = cot + times_transposed(recv_grad, a_recv_v[...]) + times_transposed(send_grad, a_send_v[...])
        swap_wait(2, back_send, back_recv)
        grad_ref[0] = local_grad[...] + dot(pick_halo, back_recv[...].reshape(padded, width))

    if not fused:
        store_part(1, inner_rows(latent, recv_grad))
        store_part(0, inner_rows(halo, halo_grad) + inner_rows(latent, send_grad))
        finish_mesh()
        return

    store_part(1, inner_rows(latent, recv_grad))
    send_pairs(width)
    store_part(0, inner_rows(halo, halo_grad) + inner_rows(latent, send_grad))
    send_pairs(0)
    order = [lines - 1] + list(range(lines - 1))
    for row in order[1:]:
        stage_row(row)
    finish_mesh()

    own_rows = pl.ds(pl.multiple_of(far * quarter, TILE), quarter)

    def finish_row():
        total = line_send[line].astype(F32)
        for step in range(1, lines):
            row = lax.rem(line + step, lines)
            line_copy(row, row).wait_recv()
            total = total + line_recv[row].astype(F32)
        last_send[...] = total.astype(BF)
        for k in (2, 0, 1):
            last_copy(k).start()

    for row in order:
        total = staged[COLUMNS * row + column, own_rows, :].astype(F32)
        for k in range(3):
            plane_copy(row, k).wait()
            total = total + plane_recv[row, k].astype(F32)
        line_send[row] = total.astype(BF)

        @pl.when(line != row)
        def _():
            line_copy(row, line).start()

        if row == lines - 2:
            pl.when(line != 0)(finish_row)
        if row == lines - 3:
            pl.when(line == 0)(finish_row)

    def place(k, value):
        dx, dc = steps[k] if k >= 0 else (0, 0)
        start = lax.rem(half + dc, 2) * unit + lax.rem(far + dx, 2) * quarter
        weights_ref[pl.ds(pl.multiple_of(start, TILE), quarter), :] = value

    place(-1, last_send[...].astype(F32))
    for step in range(1, lines):
        row = lax.rem(line + step, lines)
        line_copy(row, row).wait_send()
    for k in (1, 0, 2):
        last_copy(k).wait()
        place(k, last_recv[k].astype(F32))


def hand_over(*refs):
    sources, targets, sem = refs[:3], refs[3:6], refs[6]
    copies = [pltpu.make_async_copy(sources[i], targets[i], sem.at[i]) for i in range(3)]
    for copy in copies:
        copy.start()
    for copy in copies:
        copy.wait()


def on_device(
    grid_in, mesh_init, g2m_geometry, w_embed, w_g2m, w_geo, a_send, a_recv, b_node, cotangent,
    g2m_send_rows, g2m_counts, g2m_senders, g2m_receivers, mesh_send_rows, mesh_senders, mesh_receivers,
):
    groups = lax.axis_size("graph")
    samples = lax.axis_size("sample")
    slots = g2m_send_rows.shape[2]
    halos = mesh_send_rows.shape[2]
    width = w_g2m.shape[1]
    mesh_rows = mesh_init.shape[1]
    block_rows = 3 * width // groups
    fused = samples == 4 and groups % COLUMNS == 0 and groups > 2 * COLUMNS and block_rows % (4 * TILE) == 0
    unit = block_rows // 2 if fused else TILE
    weights_shape = (block_rows, width) if fused else (3 * width, width)
    edges, mesh_edges = g2m_senders.shape[0], mesh_senders.shape[0]
    one = groups if fused else 1
    quarter = unit // 2 if fused else TILE
    lines = groups // COLUMNS if fused else 1
    vmem = pl.BlockSpec(memory_space=pltpu.VMEM)
    hbm = pl.BlockSpec(memory_space=pltpu.HBM)
    slab = pltpu.VMEM((groups, PAD, width), BF)
    held = pltpu.VMEM if fused else jax.ShapeDtypeStruct
    small = (
        g2m_send_rows, g2m_counts, jnp.swapaxes(mesh_send_rows, 1, 2), g2m_senders[None], g2m_receivers[None],
        mesh_senders[None], mesh_receivers[None], g2m_geometry, w_geo,
    )
    mesh_out, grad_mesh, weights = pl.pallas_call(
        functools.partial(kernel, (groups, slots, halos, fused)),
        out_shape=(held(mesh_init.shape, BF), held(mesh_init.shape, F32), held(weights_shape, F32)),
        in_specs=[hbm] * 17,
        out_specs=(vmem, vmem, vmem),
        scratch_shapes=[pltpu.VMEM(value.shape, value.dtype) for value in small]
        + [
            pltpu.VMEM(grid_in.shape[1:], BF), pltpu.VMEM(mesh_init.shape[1:], BF),
            pltpu.VMEM(w_embed.shape, BF), pltpu.VMEM(w_g2m.shape, BF), pltpu.VMEM(a_send.shape, BF),
            pltpu.VMEM(a_recv.shape, BF), pltpu.VMEM(b_node.shape, BF), pltpu.VMEM(cotangent.shape[1:], BF),
            slab, slab, slab, slab, slab, slab,
            pltpu.VMEM((edges, width), F32), pltpu.VMEM((mesh_edges, width), F32),
            pltpu.VMEM((mesh_rows, width), F32),
            pltpu.VMEM((3 * width, width) if fused else (TILE, width), BF),
            pltpu.VMEM((one, unit, width), BF), pltpu.VMEM((one, unit, width), BF),
            pltpu.VMEM((lines, 3, quarter, width), BF), pltpu.VMEM((lines, quarter, width), BF),
            pltpu.VMEM((lines, quarter, width), BF), pltpu.VMEM((quarter, width), BF), pltpu.VMEM((3, quarter, width), BF),
            pltpu.SemaphoreType.DMA((8,)), pltpu.SemaphoreType.DMA((9,)), pltpu.SemaphoreType.DMA((3, groups)), pltpu.SemaphoreType.DMA((3, groups)),
            pltpu.SemaphoreType.DMA((2, groups)), pltpu.SemaphoreType.DMA((2, lines, 3)),
            pltpu.SemaphoreType.DMA((2, lines)), pltpu.SemaphoreType.DMA((2, 3)),
        ],
        compiler_params=pltpu.CompilerParams(
            collective_id=0, has_side_effects=True, vmem_limit_bytes=LIMIT
        ),
    )(
        *small, grid_in, mesh_init, w_embed, w_g2m, a_send, a_recv, b_node, cotangent,
    )
    if not fused:
        weights = lax.psum(lax.psum_scatter(weights, "graph", scatter_dimension=0, tiled=True), "sample")
        return mesh_out, grad_mesh, weights
    results = tuple(pltpu.with_memory_space_constraint(value, pltpu.VMEM) for value in (mesh_out, grad_mesh, weights))
    return pl.pallas_call(
        hand_over,
        out_shape=tuple(jax.ShapeDtypeStruct(value.shape, value.dtype) for value in results),
        in_specs=[vmem] * 3,
        out_specs=(hbm,) * 3,
        scratch_shapes=[pltpu.SemaphoreType.DMA((3,))],
    )(*results)


def solution(mesh):
    rows = P("sample", "graph", None)
    placed = (
        rows, rows, P(None, "graph"), P(), P(), P(), P(), P(), P(), rows,
        P("graph", None, None), P("graph", None), P("graph"), P("graph"), P("graph", None, None), P("graph"), P("graph"),
    )
    return jax.shard_map(
        on_device, mesh=mesh, in_specs=placed, out_specs=(rows, rows, P("graph", None)), check_vma=False
    )
```

```python
import functools

import jax
import jax.numpy as jnp
from jax import lax
from jax.experimental import pallas as pl
from jax.experimental.pallas import tpu as pltpu
from jax.sharding import PartitionSpec as P

PAD = 8
TILE = 16
LIMIT = 67043328 - 1024 * 1024
COLUMNS = 2
BF = jnp.bfloat16
F32 = jnp.float32


def logistic(v):
    return 0.5 + 0.5 * jnp.tanh(0.5 * v)


def dot(left, right):
    return jnp.dot(left, right, preferred_element_type=F32)


def times_transposed(left, right):
    return lax.dot_general(left, right, (((1,), (1,)), ((), ())), preferred_element_type=F32)


def inner_rows(left, right):
    return lax.dot_general(left, right, (((0,), (0,)), ((), ())), preferred_element_type=F32)


def hot(rows, index_row):
    shape = (rows, index_row.shape[1])
    return jnp.where(lax.broadcasted_iota(jnp.int32, shape, 0) == index_row, 1.0, 0.0).astype(BF)


def two_terms(values):
    high = values.astype(BF)
    return jnp.concatenate([high, (values - high.astype(F32)).astype(BF)], axis=0)


def repack(position, count):
    return position if count == PAD else position + lax.div(position, count) * (PAD - count)


def spread(table, pattern):
    low = lax.rem(table, 256)
    return dot(lax.div(table, 256).astype(BF), pattern) * 256.0 + dot(low.astype(BF), pattern)


def slot_rows(grid_rows_ref, counts_ref, halo_rows_ref, groups, padded, halos):
    def grid_of(rows):
        row = lax.broadcasted_iota(jnp.int32, (rows, padded), 0)
        return row, lax.broadcasted_iota(jnp.int32, (rows, padded), 1)

    peer, column = grid_of(groups)
    by_peer = lax.div(column, PAD) == peer
    peer_hot = jnp.where(by_peer, 1.0, 0.0).astype(BF)
    slot, column = grid_of(grid_rows_ref.shape[2])
    slot_hot = jnp.where(lax.rem(column, PAD) == slot, 1.0, 0.0).astype(BF)
    picked = jnp.sum(jnp.where(by_peer, spread(grid_rows_ref[0], slot_hot), 0.0), axis=0, keepdims=True)
    live = dot(counts_ref[...].astype(BF), peer_hot)
    _, column = grid_of(1)
    position = lax.rem(column, PAD)
    grid_rows = jnp.where(position.astype(F32) < live, picked, -1.0).astype(jnp.int32)
    slot, column = grid_of(halos)
    by_slot = lax.rem(column, PAD) == slot
    picked = jnp.sum(jnp.where(by_slot, spread(halo_rows_ref[0], peer_hot), 0.0), axis=0, keepdims=True)
    halo_rows = jnp.where(position < halos, picked, -1.0).astype(jnp.int32)
    return grid_rows, halo_rows


def kernel(
    cfg,
    grid_rows_hbm, counts_hbm, halo_rows_hbm, g2m_senders_hbm, g2m_receivers_hbm, mesh_senders_hbm, mesh_receivers_hbm,
    geom_hbm, w_geo_hbm,
    grid_hbm, init_hbm, w_embed_hbm, w_g2m_hbm, a_send_hbm, a_recv_hbm, b_node_hbm, cot_hbm,
    out_ref, grad_ref, weights_ref,
    grid_rows_ref, counts_ref, halo_rows_ref, g2m_senders_ref, g2m_receivers_ref, mesh_senders_ref, mesh_receivers_ref,
    geom_ref, w_geo_ref,
    grid_v, init_v, w_embed_v, w_g2m_v, a_send_v, a_recv_v, b_node_v, cot_v,
    lat_send, lat_recv, halo_send, halo_recv, back_send, back_recv,
    geo_part, slope_v, local_grad, grads, pair_recv, staged, plane_recv, line_send, line_recv, last_send, last_recv,
    load_sem, small_sem, g_send_sem, g_recv_sem, pair_sem, plane_sem, line_sem, last_sem,
):
    groups, slots, halos, fused = cfg
    me = lax.axis_index("graph")
    sample = lax.axis_index("sample")
    half = lax.rem(sample, 2)
    far = lax.div(sample, 2)
    column = lax.rem(me, COLUMNS)
    line = lax.div(me, COLUMNS)
    core_peer = sample + 1 - 2 * half

    def sample_at(dx, dc):
        return 2 * lax.rem(far + dx, 2) + lax.rem(half + dc, 2)

    small = [
        pltpu.make_async_copy(src, dst, small_sem.at[i])
        for i, (src, dst) in enumerate(
            [
                (grid_rows_hbm, grid_rows_ref), (counts_hbm, counts_ref), (halo_rows_hbm, halo_rows_ref),
                (g2m_senders_hbm, g2m_senders_ref), (g2m_receivers_hbm, g2m_receivers_ref),
                (mesh_senders_hbm, mesh_senders_ref), (mesh_receivers_hbm, mesh_receivers_ref),
                (geom_hbm, geom_ref), (w_geo_hbm, w_geo_ref),
            ]
        )
    ]
    for copy in small[:3]:
        copy.start()
    loads = []
    for i, (src, dst) in enumerate(
        [
            (grid_hbm.at[0], grid_v), (w_embed_hbm, w_embed_v), (w_g2m_hbm, w_g2m_v),
            (init_hbm.at[0], init_v), (a_send_hbm, a_send_v), (a_recv_hbm, a_recv_v),
            (b_node_hbm, b_node_v), (cot_hbm.at[0], cot_v),
        ]
    ):
        copy = pltpu.make_async_copy(src, dst, load_sem.at[i])
        if i < 2:
            copy.start()
        loads.append(copy)
    ld_grid, ld_embed, ld_g2m, ld_init, ld_asend, ld_arecv, ld_bnode, ld_cot = loads

    barrier = pltpu.get_barrier_semaphore()

    def greet(step, carry):
        pl.semaphore_signal(barrier, inc=1, device_id={"graph": lax.rem(me + step, groups)}, device_id_type=pl.DeviceIdType.MESH)
        return carry

    lax.fori_loop(1, groups, greet, 0)
    greeted = groups - 1
    if fused:
        other_column = COLUMNS * line + lax.rem(column + 1, COLUMNS)
        for graph, peer in ((me, core_peer), (me, sample_at(1, 0)), (me, sample_at(1, 1)), (other_column, sample_at(1, 0))):
            pl.semaphore_signal(
                barrier, inc=1, device_id={"graph": graph, "sample": peer}, device_id_type=pl.DeviceIdType.MESH
            )
        greeted += 4

    def swap_copy(kind, src, dst, peer, slot):
        return pltpu.make_async_remote_copy(
            src_ref=src, dst_ref=dst, send_sem=g_send_sem.at[kind, peer], recv_sem=g_recv_sem.at[kind, slot],
            device_id={"graph": peer}, device_id_type=pl.DeviceIdType.MESH,
        )

    def swap_start(kind, source, target):
        def body(step, carry):
            peer = lax.rem(me + step, groups)
            swap_copy(kind, source.at[peer], target.at[me], peer, me).start()
            return carry

        lax.fori_loop(1, groups, body, 0)

    def swap_wait(kind, source, target):
        def body(step, carry):
            peer = lax.rem(me + step, groups)
            swap_copy(kind, source.at[peer], target.at[peer], peer, peer).wait()
            return carry

        lax.fori_loop(1, groups, body, 0)

    width = w_g2m_v.shape[1]
    mesh_rows = init_v.shape[0]
    padded = groups * PAD
    for copy in small[:3]:
        copy.wait()
    for copy in small[3:] + loads[2:4]:
        copy.start()
    grid_rows, halo_rows = slot_rows(grid_rows_ref, counts_ref, halo_rows_ref, groups, padded, halos)

    pick_grid = hot(grid_v.shape[0], grid_rows)
    ld_grid.wait()
    chosen = inner_rows(pick_grid, grid_v[...]).astype(BF)
    ld_embed.wait()
    for copy in loads[4:]:
        copy.start()
    embedded = dot(chosen, w_embed_v[...])
    lat_send[...] = (embedded * logistic(embedded)).astype(BF).reshape(groups, PAD, width)
    pl.semaphore_wait(barrier, greeted)
    swap_start(0, lat_send, lat_recv)
    lat_recv[me] = lat_send[me]
    for copy in small[3:]:
        copy.wait()
    geo_part[...] = inner_rows(geom_ref[...], w_geo_ref[...])
    grid_hot = hot(padded, repack(g2m_senders_ref[...], slots))
    recv_hot_g = hot(mesh_rows, g2m_receivers_ref[...])
    ld_g2m.wait()
    ld_init.wait()
    swap_wait(0, lat_send, lat_recv)
    grid_proj = dot(lat_recv[...].reshape(padded, width), w_g2m_v[...])
    grid_proj = two_terms(grid_proj)
    grid_hot = jnp.concatenate([grid_hot, grid_hot], axis=0)
    summed = init_v[...].astype(F32)
    edges = grid_hot.shape[1]
    chunk = 256 if edges % 256 == 0 else edges
    for first in range(0, edges, chunk):
        v = inner_rows(grid_hot[:, first : first + chunk], grid_proj) + geo_part[first : first + chunk, :]
        message = (v * logistic(v)).astype(BF)
        summed = summed + dot(recv_hot_g[:, first : first + chunk], message)
    latent = summed.astype(BF)

    pick_halo = hot(mesh_rows, halo_rows)
    halo_send[...] = inner_rows(pick_halo, latent).astype(BF).reshape(groups, PAD, width)
    swap_start(1, halo_send, halo_recv)
    halo_recv[me] = halo_send[me]
    ld_asend.wait()
    ld_arecv.wait()
    recv_proj = dot(latent, a_recv_v[...])
    local_proj = dot(latent, a_send_v[...])
    recv_hot = hot(mesh_rows, mesh_receivers_ref[...])
    table_row = mesh_senders_ref[...]
    table_row = jnp.where(
        table_row < groups * halos, repack(table_row, halos), table_row + (padded - groups * halos)
    )
    send_hot = hot(padded + mesh_rows, table_row)
    ld_bnode.wait()
    ld_cot.wait()
    swap_wait(1, halo_send, halo_recv)
    halo = halo_recv[...].reshape(padded, width)
    halo_proj = dot(halo, a_send_v[...])
    all_proj = two_terms(jnp.concatenate([halo_proj, local_proj, recv_proj], axis=0))
    all_hot = jnp.concatenate([send_hot, recv_hot], axis=0)
    twice_hot = jnp.concatenate([all_hot, all_hot], axis=0)
    mesh_edges = recv_hot.shape[1]
    chunk = 256 if mesh_edges % 256 == 0 else mesh_edges
    agg = jnp.zeros((mesh_rows, width), F32)
    for first in range(0, mesh_edges, chunk):
        v = inner_rows(twice_hot[:, first : first + chunk], all_proj)
        s = logistic(v)
        slope_v[first : first + chunk, :] = s * (1.0 + v * (1.0 - s))
        agg = agg + dot(recv_hot[:, first : first + chunk], (v * s).astype(BF))
    aggregate = agg.astype(BF)
    update = dot(aggregate, b_node_v[...])
    s = logistic(update)
    out_ref[0] = (latent.astype(F32) + update * s).astype(BF)
    cot = cot_v[...].astype(F32)
    d_update = (cot * (s * (1.0 + update * (1.0 - s)))).astype(BF)
    d_aggregate = times_transposed(d_update, b_node_v[...]).astype(BF)

    kind = BF if fused else F32
    target = grads if fused else weights_ref
    unit = staged.shape[2]
    waiting = list(range(groups))

    def rows_of(block, side):
        return pl.ds(pl.multiple_of((2 * block + side) * unit, TILE), unit)

    def pair_copy(block):
        return pltpu.make_async_remote_copy(
            src_ref=grads.at[rows_of(block, 1 - half)], dst_ref=pair_recv.at[block],
            send_sem=pair_sem.at[0, block], recv_sem=pair_sem.at[1, block],
            device_id={"sample": core_peer}, device_id_type=pl.DeviceIdType.MESH,
        )

    def store_part(number, value):
        target[number * width : (number + 1) * width, :] = value.astype(kind)

    def send_pairs(first, past):
        for block in [b for b in waiting if first <= b * 2 * unit and (b + 1) * 2 * unit <= past]:
            waiting.remove(block)
            pair_copy(block).start()

    quarter = unit // 2
    lines = groups // COLUMNS
    steps = [(1, 0), (0, 1), (1, 1)]

    def plane_copy(row, part, k):
        dx, dy = steps[k]
        x, y = lax.rem(far + dx, 2), lax.rem(column + dy, COLUMNS)
        return pltpu.make_async_remote_copy(
            src_ref=staged.at[COLUMNS * row + y, part, pl.ds(pl.multiple_of(x * quarter, TILE), quarter)],
            dst_ref=plane_recv.at[row, part, k],
            send_sem=plane_sem.at[0, row, part, k], recv_sem=plane_sem.at[1, row, part, k],
            device_id={"graph": COLUMNS * line + y, "sample": 2 * x + half}, device_id_type=pl.DeviceIdType.MESH,
        )

    def line_copy(row, part, slot):
        return pltpu.make_async_remote_copy(
            src_ref=line_send.at[row, part], dst_ref=line_recv.at[slot, part],
            send_sem=line_sem.at[0, row, part], recv_sem=line_sem.at[1, slot, part],
            device_id={"graph": COLUMNS * row + column}, device_id_type=pl.DeviceIdType.MESH,
        )

    def last_copy(part, k):
        return pltpu.make_async_remote_copy(
            src_ref=last_send.at[part], dst_ref=last_recv.at[part, k],
            send_sem=last_sem.at[0, part, k], recv_sem=last_sem.at[1, part, k],
            device_id={"sample": sample_at(*steps[k])}, device_id_type=pl.DeviceIdType.MESH,
        )

    parts = staged.shape[1] if fused else 1
    lanes = width // parts

    def columns_of(part):
        return pl.ds(part * lanes, lanes)

    def stage_row(row, which):
        for block in range(COLUMNS * row, COLUMNS * (row + 1)):
            if which[0] == 0:
                pair_copy(block).wait()
            for part in which:
                staged[block, part] = (
                    grads[rows_of(block, half), columns_of(part)].astype(F32)
                    + pair_recv[block, :, columns_of(part)].astype(F32)
                ).astype(BF)
        for part in which:
            for k in (2, 0, 1):
                plane_copy(row, part, k).start()

    store_part(2, inner_rows(aggregate, d_update))
    if fused:
        send_pairs(2 * width, 3 * width)
    d_both = jnp.zeros((padded + 2 * mesh_rows, width), F32)
    for first in range(0, mesh_edges, chunk):
        d_pre = (inner_rows(recv_hot[:, first : first + chunk], d_aggregate) * slope_v[first : first + chunk, :]).astype(BF)
        d_both = d_both + dot(all_hot[:, first : first + chunk], d_pre)
    d_both = d_both.astype(BF)
    halo_grad = d_both[:padded]
    send_grad = d_both[padded : padded + mesh_rows]
    recv_grad = d_both[padded + mesh_rows :]
    if fused:
        store_part(0, inner_rows(halo, halo_grad) + inner_rows(latent, send_grad))
        send_pairs(0, width)
        store_part(1, inner_rows(latent, recv_grad))
        send_pairs(0, 3 * width)
        stage_row(lines - 1, [0])
    back_send[...] = times_transposed(halo_grad, a_send_v[...]).astype(BF).reshape(groups, PAD, width)
    swap_start(2, back_send, back_recv)
    back_recv[me] = back_send[me]

    def finish_mesh():
        local_grad[...] = cot + times_transposed(recv_grad, a_recv_v[...]) + times_transposed(send_grad, a_send_v[...])
        swap_wait(2, back_send, back_recv)
        grad_ref[0] = local_grad[...] + dot(pick_halo, back_recv[...].reshape(padded, width))

    if not fused:
        store_part(1, inner_rows(latent, recv_grad))
        store_part(0, inner_rows(halo, halo_grad) + inner_rows(latent, send_grad))
        finish_mesh()
        return

    every = list(range(parts))
    for row in range(lines - 1):
        stage_row(row, every)
        if row == 0 and parts > 1:
            stage_row(lines - 1, every[1:])
    finish_mesh()

    own_rows = pl.ds(pl.multiple_of(far * quarter, TILE), quarter)

    def finish_row():
        for part in every:
            total = line_send[line, part].astype(F32)
            for step in range(1, lines):
                row = lax.rem(line + step, lines)
                line_copy(row, part, row).wait_recv()
                total = total + line_recv[row, part].astype(F32)
            last_send[part] = total.astype(BF)
            for k in (2, 0, 1):
                last_copy(part, k).start()

    order = [(lines - 1, 0)] + [(0, part) for part in every] + [(lines - 1, part) for part in every[1:]]
    order += [(row, part) for row in range(1, lines - 1) for part in every]
    for row, part in order:
        total = staged[COLUMNS * row + column, part, own_rows, :].astype(F32)
        for k in range(3):
            plane_copy(row, part, k).wait()
            total = total + plane_recv[row, part, k].astype(F32)
        line_send[row, part] = total.astype(BF)

        @pl.when(line != row)
        def _():
            line_copy(row, part, line).start()

        if (row, part) == (lines - 2, 0):
            pl.when(line == 0)(finish_row)
    pl.when(line != 0)(finish_row)

    def place(k, part, value):
        dx, dc = steps[k] if k >= 0 else (0, 0)
        start = lax.rem(half + dc, 2) * unit + lax.rem(far + dx, 2) * quarter
        weights_ref[pl.ds(pl.multiple_of(start, TILE), quarter), columns_of(part)] = value.astype(F32)

    for part in every:
        place(-1, part, last_send[part])
        for step in range(1, lines):
            row = lax.rem(line + step, lines)
            line_copy(row, part, row).wait_send()
    for part in every:
        for k in (1, 0, 2):
            last_copy(part, k).wait()
            place(k, part, last_recv[part, k])


def hand_over(*refs):
    sources, targets, sem = refs[:3], refs[3:6], refs[6]
    copies = [pltpu.make_async_copy(sources[i], targets[i], sem.at[i]) for i in range(3)]
    for copy in copies:
        copy.start()
    for copy in copies:
        copy.wait()


def on_device(
    grid_in, mesh_init, g2m_geometry, w_embed, w_g2m, w_geo, a_send, a_recv, b_node, cotangent,
    g2m_send_rows, g2m_counts, g2m_senders, g2m_receivers, mesh_send_rows, mesh_senders, mesh_receivers,
):
    groups = lax.axis_size("graph")
    samples = lax.axis_size("sample")
    slots = g2m_send_rows.shape[2]
    halos = mesh_send_rows.shape[2]
    width = w_g2m.shape[1]
    mesh_rows = mesh_init.shape[1]
    block_rows = 3 * width // groups
    fused = samples == 4 and groups % COLUMNS == 0 and groups > 2 * COLUMNS and block_rows % (4 * TILE) == 0
    unit = block_rows // 2 if fused else TILE
    weights_shape = (block_rows, width) if fused else (3 * width, width)
    edges, mesh_edges = g2m_senders.shape[0], mesh_senders.shape[0]
    one = groups if fused else 1
    quarter = unit // 2 if fused else TILE
    lines = groups // COLUMNS if fused else 1
    parts = 2 if width % 256 == 0 else 1
    lanes = width // parts
    vmem = pl.BlockSpec(memory_space=pltpu.VMEM)
    hbm = pl.BlockSpec(memory_space=pltpu.HBM)
    slab = pltpu.VMEM((groups, PAD, width), BF)
    held = pltpu.VMEM if fused else jax.ShapeDtypeStruct
    small = (
        g2m_send_rows, g2m_counts, jnp.swapaxes(mesh_send_rows, 1, 2), g2m_senders[None], g2m_receivers[None],
        mesh_senders[None], mesh_receivers[None], g2m_geometry, w_geo,
    )
    mesh_out, grad_mesh, weights = pl.pallas_call(
        functools.partial(kernel, (groups, slots, halos, fused)),
        out_shape=(held(mesh_init.shape, BF), held(mesh_init.shape, F32), held(weights_shape, F32)),
        in_specs=[hbm] * 17,
        out_specs=(vmem, vmem, vmem),
        scratch_shapes=[pltpu.VMEM(value.shape, value.dtype) for value in small]
        + [
            pltpu.VMEM(grid_in.shape[1:], BF), pltpu.VMEM(mesh_init.shape[1:], BF),
            pltpu.VMEM(w_embed.shape, BF), pltpu.VMEM(w_g2m.shape, BF), pltpu.VMEM(a_send.shape, BF),
            pltpu.VMEM(a_recv.shape, BF), pltpu.VMEM(b_node.shape, BF), pltpu.VMEM(cotangent.shape[1:], BF),
            slab, slab, slab, slab, slab, slab,
            pltpu.VMEM((edges, width), F32), pltpu.VMEM((mesh_edges, width), F32),
            pltpu.VMEM((mesh_rows, width), F32),
            pltpu.VMEM((3 * width, width) if fused else (TILE, width), BF),
            pltpu.VMEM((one, unit, width), BF), pltpu.VMEM((one, parts, unit, lanes), BF),
            pltpu.VMEM((lines, parts, 3, quarter, lanes), BF), pltpu.VMEM((lines, parts, quarter, lanes), BF),
            pltpu.VMEM((lines, parts, quarter, lanes), BF), pltpu.VMEM((parts, quarter, lanes), BF),
            pltpu.VMEM((parts, 3, quarter, lanes), BF),
            pltpu.SemaphoreType.DMA((8,)), pltpu.SemaphoreType.DMA((9,)), pltpu.SemaphoreType.DMA((3, groups)), pltpu.SemaphoreType.DMA((3, groups)),
            pltpu.SemaphoreType.DMA((2, groups)), pltpu.SemaphoreType.DMA((2, lines, parts, 3)),
            pltpu.SemaphoreType.DMA((2, lines, parts)), pltpu.SemaphoreType.DMA((2, parts, 3)),
        ],
        compiler_params=pltpu.CompilerParams(
            collective_id=0, has_side_effects=True, vmem_limit_bytes=LIMIT
        ),
    )(
        *small, grid_in, mesh_init, w_embed, w_g2m, a_send, a_recv, b_node, cotangent,
    )
    if not fused:
        weights = lax.psum(lax.psum_scatter(weights, "graph", scatter_dimension=0, tiled=True), "sample")
        return mesh_out, grad_mesh, weights
    results = tuple(pltpu.with_memory_space_constraint(value, pltpu.VMEM) for value in (mesh_out, grad_mesh, weights))
    return pl.pallas_call(
        hand_over,
        out_shape=tuple(jax.ShapeDtypeStruct(value.shape, value.dtype) for value in results),
        in_specs=[vmem] * 3,
        out_specs=(hbm,) * 3,
        scratch_shapes=[pltpu.SemaphoreType.DMA((3,))],
    )(*results)


def solution(mesh):
    rows = P("sample", "graph", None)
    placed = (
        rows, rows, P(None, "graph"), P(), P(), P(), P(), P(), P(), rows,
        P("graph", None, None), P("graph", None), P("graph"), P("graph"), P("graph", None, None), P("graph"), P("graph"),
    )
    return jax.shard_map(
        on_device, mesh=mesh, in_specs=placed, out_specs=(rows, rows, P("graph", None)), check_vma=False
    )
```

```python
import functools

import jax
import jax.numpy as jnp
from jax import lax
from jax.experimental import pallas as pl
from jax.experimental.pallas import tpu as pltpu
from jax.sharding import PartitionSpec as P

PAD = 8
TILE = 16
LIMIT = 67043328 - 1024 * 1024
COLUMNS = 2
BF = jnp.bfloat16
F32 = jnp.float32


def logistic(v):
    return 0.5 + 0.5 * jnp.tanh(0.5 * v)


def dot(left, right):
    return jnp.dot(left, right, preferred_element_type=F32)


def times_transposed(left, right):
    return lax.dot_general(left, right, (((1,), (1,)), ((), ())), preferred_element_type=F32)


def inner_rows(left, right):
    return lax.dot_general(left, right, (((0,), (0,)), ((), ())), preferred_element_type=F32)


def hot(rows, index_row):
    shape = (rows, index_row.shape[1])
    return jnp.where(lax.broadcasted_iota(jnp.int32, shape, 0) == index_row, 1.0, 0.0).astype(BF)


def two_terms(values):
    high = values.astype(BF)
    return jnp.concatenate([high, (values - high.astype(F32)).astype(BF)], axis=0)


def repack(position, count):
    return position if count == PAD else position + lax.div(position, count) * (PAD - count)


def spread(table, pattern):
    low = lax.rem(table, 256)
    return dot(lax.div(table, 256).astype(BF), pattern) * 256.0 + dot(low.astype(BF), pattern)


def wait_bytes(ref, sem):
    pltpu.make_async_copy(ref, ref, sem).wait()


def slot_rows(grid_rows_ref, counts_ref, halo_rows_ref, groups, padded, halos):
    def grid_of(rows):
        row = lax.broadcasted_iota(jnp.int32, (rows, padded), 0)
        return row, lax.broadcasted_iota(jnp.int32, (rows, padded), 1)

    peer, column = grid_of(groups)
    by_peer = lax.div(column, PAD) == peer
    peer_hot = jnp.where(by_peer, 1.0, 0.0).astype(BF)
    slot, column = grid_of(grid_rows_ref.shape[2])
    slot_hot = jnp.where(lax.rem(column, PAD) == slot, 1.0, 0.0).astype(BF)
    picked = jnp.sum(jnp.where(by_peer, spread(grid_rows_ref[0], slot_hot), 0.0), axis=0, keepdims=True)
    live = dot(counts_ref[...].astype(BF), peer_hot)
    _, column = grid_of(1)
    position = lax.rem(column, PAD)
    grid_rows = jnp.where(position.astype(F32) < live, picked, -1.0).astype(jnp.int32)
    slot, column = grid_of(halos)
    by_slot = lax.rem(column, PAD) == slot
    picked = jnp.sum(jnp.where(by_slot, spread(halo_rows_ref[0], peer_hot), 0.0), axis=0, keepdims=True)
    halo_rows = jnp.where(position < halos, picked, -1.0).astype(jnp.int32)
    return grid_rows, halo_rows


def kernel(
    cfg,
    grid_rows_hbm, counts_hbm, halo_rows_hbm, g2m_senders_hbm, g2m_receivers_hbm, mesh_senders_hbm, mesh_receivers_hbm,
    geom_hbm, w_geo_hbm,
    grid_hbm, init_hbm, w_embed_hbm, w_g2m_hbm, a_send_hbm, a_recv_hbm, b_node_hbm, cot_hbm,
    out_ref, grad_ref, weights_ref,
    grid_rows_ref, counts_ref, halo_rows_ref, g2m_senders_ref, g2m_receivers_ref, mesh_senders_ref, mesh_receivers_ref,
    geom_ref, w_geo_ref,
    grid_v, init_v, w_embed_v, w_g2m_v, a_send_v, a_recv_v, b_node_v, cot_v,
    lat_send, lat_recv, halo_send, halo_recv, back_send, back_recv,
    geo_part, slope_v, local_grad, grads, pair_recv, staged, plane_recv, line_send, line_recv, last_send, last_recv,
    load_sem, small_sem, swap_sem, pair_sem, plane_sem, line_sem, last_sem,
):
    groups, slots, halos, fused = cfg
    me = lax.axis_index("graph")
    sample = lax.axis_index("sample")
    half = lax.rem(sample, 2)
    far = lax.div(sample, 2)
    column = lax.rem(me, COLUMNS)
    line = lax.div(me, COLUMNS)
    core_peer = sample + 1 - 2 * half

    def sample_at(dx, dc):
        return 2 * lax.rem(far + dx, 2) + lax.rem(half + dc, 2)

    small = [
        pltpu.make_async_copy(src, dst, small_sem.at[i])
        for i, (src, dst) in enumerate(
            [
                (grid_rows_hbm, grid_rows_ref), (counts_hbm, counts_ref), (halo_rows_hbm, halo_rows_ref),
                (g2m_senders_hbm, g2m_senders_ref), (g2m_receivers_hbm, g2m_receivers_ref),
                (mesh_senders_hbm, mesh_senders_ref), (mesh_receivers_hbm, mesh_receivers_ref),
                (geom_hbm, geom_ref), (w_geo_hbm, w_geo_ref),
            ]
        )
    ]
    for copy in small[:3]:
        copy.start()
    loads = []
    for i, (src, dst) in enumerate(
        [
            (grid_hbm.at[0], grid_v), (w_embed_hbm, w_embed_v), (w_g2m_hbm, w_g2m_v),
            (init_hbm.at[0], init_v), (a_send_hbm, a_send_v), (a_recv_hbm, a_recv_v),
            (b_node_hbm, b_node_v), (cot_hbm.at[0], cot_v),
        ]
    ):
        copy = pltpu.make_async_copy(src, dst, load_sem.at[i])
        if i < 2:
            copy.start()
        loads.append(copy)
    ld_grid, ld_embed, ld_g2m, ld_init, ld_asend, ld_arecv, ld_bnode, ld_cot = loads

    barrier = pltpu.get_barrier_semaphore()

    def greet(step, carry):
        pl.semaphore_signal(barrier, inc=1, device_id={"graph": lax.rem(me + step, groups)}, device_id_type=pl.DeviceIdType.MESH)
        return carry

    lax.fori_loop(1, groups, greet, 0)
    greeted = groups - 1
    if fused:
        other_column = COLUMNS * line + lax.rem(column + 1, COLUMNS)
        for graph, peer in ((me, core_peer), (me, sample_at(1, 0)), (me, sample_at(1, 1)), (other_column, sample_at(1, 0))):
            pl.semaphore_signal(
                barrier, inc=1, device_id={"graph": graph, "sample": peer}, device_id_type=pl.DeviceIdType.MESH
            )
        greeted += 4

    def swap_start(kind, source, target):
        def body(step, carry):
            peer = lax.rem(me + step, groups)
            pltpu.make_async_remote_copy(
                src_ref=source.at[peer], dst_ref=target.at[me], send_sem=swap_sem.at[0, kind], recv_sem=swap_sem.at[1, kind],
                device_id={"graph": peer}, device_id_type=pl.DeviceIdType.MESH,
            ).start()
            return carry

        lax.fori_loop(1, groups, body, 0)

    def swap_wait(kind, target):
        wait_bytes(target.at[pl.ds(0, groups - 1)], swap_sem.at[1, kind])

    def swaps_sent():
        for kind, source in enumerate((lat_send, halo_send, back_send)):
            wait_bytes(source.at[pl.ds(0, groups - 1)], swap_sem.at[0, kind])

    width = w_g2m_v.shape[1]
    mesh_rows = init_v.shape[0]
    padded = groups * PAD
    for copy in small[:3]:
        copy.wait()
    for copy in small[3:] + loads[2:4]:
        copy.start()
    grid_rows, halo_rows = slot_rows(grid_rows_ref, counts_ref, halo_rows_ref, groups, padded, halos)

    pick_grid = hot(grid_v.shape[0], grid_rows)
    ld_grid.wait()
    chosen = inner_rows(pick_grid, grid_v[...]).astype(BF)
    ld_embed.wait()
    for copy in loads[4:]:
        copy.start()
    embedded = dot(chosen, w_embed_v[...])
    lat_send[...] = (embedded * logistic(embedded)).astype(BF).reshape(groups, PAD, width)
    pl.semaphore_wait(barrier, greeted)
    swap_start(0, lat_send, lat_recv)
    lat_recv[me] = lat_send[me]
    for copy in small[3:]:
        copy.wait()
    geo_part[...] = inner_rows(geom_ref[...], w_geo_ref[...])
    grid_hot = hot(padded, repack(g2m_senders_ref[...], slots))
    recv_hot_g = hot(mesh_rows, g2m_receivers_ref[...])
    ld_g2m.wait()
    ld_init.wait()
    swap_wait(0, lat_recv)
    grid_proj = dot(lat_recv[...].reshape(padded, width), w_g2m_v[...])
    grid_proj = two_terms(grid_proj)
    grid_hot = jnp.concatenate([grid_hot, grid_hot], axis=0)
    summed = init_v[...].astype(F32)
    edges = grid_hot.shape[1]
    chunk = 256 if edges % 256 == 0 else edges
    for first in range(0, edges, chunk):
        v = inner_rows(grid_hot[:, first : first + chunk], grid_proj) + geo_part[first : first + chunk, :]
        message = (v * logistic(v)).astype(BF)
        summed = summed + dot(recv_hot_g[:, first : first + chunk], message)
    latent = summed.astype(BF)

    pick_halo = hot(mesh_rows, halo_rows)
    halo_send[...] = inner_rows(pick_halo, latent).astype(BF).reshape(groups, PAD, width)
    swap_start(1, halo_send, halo_recv)
    halo_recv[me] = halo_send[me]
    ld_asend.wait()
    ld_arecv.wait()
    recv_proj = dot(latent, a_recv_v[...])
    local_proj = dot(latent, a_send_v[...])
    recv_hot = hot(mesh_rows, mesh_receivers_ref[...])
    table_row = mesh_senders_ref[...]
    table_row = jnp.where(
        table_row < groups * halos, repack(table_row, halos), table_row + (padded - groups * halos)
    )
    send_hot = hot(padded + mesh_rows, table_row)
    ld_bnode.wait()
    ld_cot.wait()
    swap_wait(1, halo_recv)
    halo = halo_recv[...].reshape(padded, width)
    halo_proj = dot(halo, a_send_v[...])
    all_proj = two_terms(jnp.concatenate([halo_proj, local_proj, recv_proj], axis=0))
    all_hot = jnp.concatenate([send_hot, recv_hot], axis=0)
    twice_hot = jnp.concatenate([all_hot, all_hot], axis=0)
    mesh_edges = recv_hot.shape[1]
    chunk = 256 if mesh_edges % 256 == 0 else mesh_edges
    agg = jnp.zeros((mesh_rows, width), F32)
    for first in range(0, mesh_edges, chunk):
        v = inner_rows(twice_hot[:, first : first + chunk], all_proj)
        s = logistic(v)
        slope_v[first : first + chunk, :] = s * (1.0 + v * (1.0 - s))
        agg = agg + dot(recv_hot[:, first : first + chunk], (v * s).astype(BF))
    aggregate = agg.astype(BF)
    update = dot(aggregate, b_node_v[...])
    s = logistic(update)
    out_ref[0] = (latent.astype(F32) + update * s).astype(BF)
    cot = cot_v[...].astype(F32)
    d_update = (cot * (s * (1.0 + update * (1.0 - s)))).astype(BF)
    d_aggregate = times_transposed(d_update, b_node_v[...]).astype(BF)

    kind = BF if fused else F32
    target = grads if fused else weights_ref
    unit = staged.shape[2]
    parts = staged.shape[1]
    lanes = width // parts
    lines = groups // COLUMNS
    waiting = list(range(groups))

    def rows_of(block, side):
        return pl.ds(pl.multiple_of((2 * block + side) * unit, TILE), unit)

    def pair_copy(block):
        return pltpu.make_async_remote_copy(
            src_ref=grads.at[rows_of(block, 1 - half)], dst_ref=pair_recv.at[block],
            send_sem=pair_sem.at[lines], recv_sem=pair_sem.at[block // COLUMNS],
            device_id={"sample": core_peer}, device_id_type=pl.DeviceIdType.MESH,
        )

    def store_part(number, value):
        target[number * width : (number + 1) * width, :] = value.astype(kind)

    def send_pairs(first, past):
        for block in [b for b in waiting if first <= b * 2 * unit and (b + 1) * 2 * unit <= past]:
            waiting.remove(block)
            pair_copy(block).start()

    quarter = unit // 2
    steps = [(1, 0), (0, 1), (1, 1)]

    def plane_copy(row, part, k):
        dx, dy = steps[k]
        x, y = lax.rem(far + dx, 2), lax.rem(column + dy, COLUMNS)
        return pltpu.make_async_remote_copy(
            src_ref=staged.at[COLUMNS * row + y, part, pl.ds(pl.multiple_of(x * quarter, TILE), quarter)],
            dst_ref=plane_recv.at[row, part, k],
            send_sem=plane_sem.at[lines, 0], recv_sem=plane_sem.at[row, part],
            device_id={"graph": COLUMNS * line + y, "sample": 2 * x + half}, device_id_type=pl.DeviceIdType.MESH,
        )

    def line_copy(row, part, slot):
        return pltpu.make_async_remote_copy(
            src_ref=line_send.at[row, part], dst_ref=line_recv.at[slot, part],
            send_sem=line_sem.at[parts], recv_sem=line_sem.at[part],
            device_id={"graph": COLUMNS * row + column}, device_id_type=pl.DeviceIdType.MESH,
        )

    def last_copy(part, k):
        return pltpu.make_async_remote_copy(
            src_ref=last_send.at[part], dst_ref=last_recv.at[part, k],
            send_sem=last_sem.at[parts], recv_sem=last_sem.at[part],
            device_id={"sample": sample_at(*steps[k])}, device_id_type=pl.DeviceIdType.MESH,
        )

    def columns_of(part):
        return pl.ds(part * lanes, lanes)

    def stage_row(row, which):
        if which[0] == 0:
            wait_bytes(pair_recv.at[pl.ds(COLUMNS * row, COLUMNS)], pair_sem.at[row])
        for block in range(COLUMNS * row, COLUMNS * (row + 1)):
            for part in which:
                staged[block, part] = (
                    grads[rows_of(block, half), columns_of(part)].astype(F32)
                    + pair_recv[block, :, columns_of(part)].astype(F32)
                ).astype(BF)
        for part in which:
            for k in (2, 0, 1):
                plane_copy(row, part, k).start()

    store_part(2, inner_rows(aggregate, d_update))
    if fused:
        send_pairs(2 * width, 3 * width)
    d_both = jnp.zeros((padded + 2 * mesh_rows, width), F32)
    for first in range(0, mesh_edges, chunk):
        d_pre = (inner_rows(recv_hot[:, first : first + chunk], d_aggregate) * slope_v[first : first + chunk, :]).astype(BF)
        d_both = d_both + dot(all_hot[:, first : first + chunk], d_pre)
    d_both = d_both.astype(BF)
    halo_grad = d_both[:padded]
    send_grad = d_both[padded : padded + mesh_rows]
    recv_grad = d_both[padded + mesh_rows :]
    if fused:
        store_part(0, inner_rows(halo, halo_grad) + inner_rows(latent, send_grad))
        send_pairs(0, width)
        store_part(1, inner_rows(latent, recv_grad))
        send_pairs(0, 3 * width)
        stage_row(lines - 1, [0])
    back_send[...] = times_transposed(halo_grad, a_send_v[...]).astype(BF).reshape(groups, PAD, width)
    swap_start(2, back_send, back_recv)
    back_recv[me] = back_send[me]

    def finish_mesh():
        local_grad[...] = cot + times_transposed(recv_grad, a_recv_v[...]) + times_transposed(send_grad, a_send_v[...])
        swap_wait(2, back_recv)
        grad_ref[0] = local_grad[...] + dot(pick_halo, back_recv[...].reshape(padded, width))

    if not fused:
        store_part(1, inner_rows(latent, recv_grad))
        store_part(0, inner_rows(halo, halo_grad) + inner_rows(latent, send_grad))
        finish_mesh()
        swaps_sent()
        return

    every = list(range(parts))
    for row in range(lines - 1):
        stage_row(row, every)
        if row == 0 and parts > 1:
            stage_row(lines - 1, every[1:])
    finish_mesh()

    own_rows = pl.ds(pl.multiple_of(far * quarter, TILE), quarter)

    def finish_row():
        for part in every:
            total = line_send[line, part].astype(F32)
            wait_bytes(line_recv.at[pl.ds(0, lines - 1), part], line_sem.at[part])
            for step in range(1, lines):
                row = lax.rem(line + step, lines)
                total = total + line_recv[row, part].astype(F32)
            last_send[part] = total.astype(BF)
            for k in (2, 0, 1):
                last_copy(part, k).start()

    order = [(lines - 1, 0)] + [(0, part) for part in every] + [(lines - 1, part) for part in every[1:]]
    order += [(row, part) for row in range(1, lines - 1) for part in every]
    for row, part in order:
        total = staged[COLUMNS * row + column, part, own_rows, :].astype(F32)
        wait_bytes(plane_recv.at[row, part], plane_sem.at[row, part])
        for k in range(3):
            total = total + plane_recv[row, part, k].astype(F32)
        line_send[row, part] = total.astype(BF)

        @pl.when(line != row)
        def _():
            line_copy(row, part, line).start()

        if (row, part) == (lines - 2, 0):
            pl.when(line == 0)(finish_row)
    pl.when(line != 0)(finish_row)

    def place(k, part, value):
        dx, dc = steps[k] if k >= 0 else (0, 0)
        start = lax.rem(half + dc, 2) * unit + lax.rem(far + dx, 2) * quarter
        weights_ref[pl.ds(pl.multiple_of(start, TILE), quarter), columns_of(part)] = value.astype(F32)

    for part in every:
        place(-1, part, last_send[part])
    swaps_sent()
    wait_bytes(pair_recv, pair_sem.at[lines])
    wait_bytes(plane_recv, plane_sem.at[lines, 0])
    wait_bytes(line_send.at[pl.ds(0, lines - 1)], line_sem.at[parts])
    for part in every:
        wait_bytes(last_recv.at[part], last_sem.at[part])
        for k in range(3):
            place(k, part, last_recv[part, k])
    wait_bytes(last_recv, last_sem.at[parts])


def hand_over(*refs):
    sources, targets, sem = refs[:3], refs[3:6], refs[6]
    copies = [pltpu.make_async_copy(sources[i], targets[i], sem.at[i]) for i in range(3)]
    for copy in copies:
        copy.start()
    for copy in copies:
        copy.wait()


def on_device(
    grid_in, mesh_init, g2m_geometry, w_embed, w_g2m, w_geo, a_send, a_recv, b_node, cotangent,
    g2m_send_rows, g2m_counts, g2m_senders, g2m_receivers, mesh_send_rows, mesh_senders, mesh_receivers,
):
    groups = lax.axis_size("graph")
    samples = lax.axis_size("sample")
    slots = g2m_send_rows.shape[2]
    halos = mesh_send_rows.shape[2]
    width = w_g2m.shape[1]
    mesh_rows = mesh_init.shape[1]
    block_rows = 3 * width // groups
    fused = samples == 4 and groups % COLUMNS == 0 and groups > 2 * COLUMNS and block_rows % (4 * TILE) == 0
    unit = block_rows // 2 if fused else TILE
    weights_shape = (block_rows, width) if fused else (3 * width, width)
    edges, mesh_edges = g2m_senders.shape[0], mesh_senders.shape[0]
    one = groups if fused else 1
    quarter = unit // 2 if fused else TILE
    lines = groups // COLUMNS if fused else 1
    parts = 2 if width % 256 == 0 else 1
    lanes = width // parts
    vmem = pl.BlockSpec(memory_space=pltpu.VMEM)
    hbm = pl.BlockSpec(memory_space=pltpu.HBM)
    slab = pltpu.VMEM((groups, PAD, width), BF)
    held = pltpu.VMEM if fused else jax.ShapeDtypeStruct
    small = (
        g2m_send_rows, g2m_counts, jnp.swapaxes(mesh_send_rows, 1, 2), g2m_senders[None], g2m_receivers[None],
        mesh_senders[None], mesh_receivers[None], g2m_geometry, w_geo,
    )
    mesh_out, grad_mesh, weights = pl.pallas_call(
        functools.partial(kernel, (groups, slots, halos, fused)),
        out_shape=(held(mesh_init.shape, BF), held(mesh_init.shape, F32), held(weights_shape, F32)),
        in_specs=[hbm] * 17,
        out_specs=(vmem, vmem, vmem),
        scratch_shapes=[pltpu.VMEM(value.shape, value.dtype) for value in small]
        + [
            pltpu.VMEM(grid_in.shape[1:], BF), pltpu.VMEM(mesh_init.shape[1:], BF),
            pltpu.VMEM(w_embed.shape, BF), pltpu.VMEM(w_g2m.shape, BF), pltpu.VMEM(a_send.shape, BF),
            pltpu.VMEM(a_recv.shape, BF), pltpu.VMEM(b_node.shape, BF), pltpu.VMEM(cotangent.shape[1:], BF),
            slab, slab, slab, slab, slab, slab,
            pltpu.VMEM((edges, width), F32), pltpu.VMEM((mesh_edges, width), F32),
            pltpu.VMEM((mesh_rows, width), F32),
            pltpu.VMEM((3 * width, width) if fused else (TILE, width), BF),
            pltpu.VMEM((one, unit, width), BF), pltpu.VMEM((one, parts, unit, lanes), BF),
            pltpu.VMEM((lines, parts, 3, quarter, lanes), BF), pltpu.VMEM((lines, parts, quarter, lanes), BF),
            pltpu.VMEM((lines, parts, quarter, lanes), BF), pltpu.VMEM((parts, quarter, lanes), BF),
            pltpu.VMEM((parts, 3, quarter, lanes), BF),
            pltpu.SemaphoreType.DMA((8,)), pltpu.SemaphoreType.DMA((9,)), pltpu.SemaphoreType.DMA((2, 3)),
            pltpu.SemaphoreType.DMA((lines + 1,)), pltpu.SemaphoreType.DMA((lines + 1, parts)),
            pltpu.SemaphoreType.DMA((parts + 1,)), pltpu.SemaphoreType.DMA((parts + 1,)),
        ],
        compiler_params=pltpu.CompilerParams(
            collective_id=0, has_side_effects=True, vmem_limit_bytes=LIMIT
        ),
    )(
        *small, grid_in, mesh_init, w_embed, w_g2m, a_send, a_recv, b_node, cotangent,
    )
    if not fused:
        weights = lax.psum(lax.psum_scatter(weights, "graph", scatter_dimension=0, tiled=True), "sample")
        return mesh_out, grad_mesh, weights
    results = tuple(pltpu.with_memory_space_constraint(value, pltpu.VMEM) for value in (mesh_out, grad_mesh, weights))
    return pl.pallas_call(
        hand_over,
        out_shape=tuple(jax.ShapeDtypeStruct(value.shape, value.dtype) for value in results),
        in_specs=[vmem] * 3,
        out_specs=(hbm,) * 3,
        scratch_shapes=[pltpu.SemaphoreType.DMA((3,))],
    )(*results)


def solution(mesh):
    rows = P("sample", "graph", None)
    placed = (
        rows, rows, P(None, "graph"), P(), P(), P(), P(), P(), P(), rows,
        P("graph", None, None), P("graph", None), P("graph"), P("graph"), P("graph", None, None), P("graph"), P("graph"),
    )
    return jax.shard_map(
        on_device, mesh=mesh, in_specs=placed, out_specs=(rows, rows, P("graph", None)), check_vma=False
    )
```
